256 devices in a mesh: job: 4 (over y), zero: 16 (over z, core), cols: 4 (over x).
Axes of the slice: x: 4, y: 4, z: 8, core: 2. Of those that a mesh axis runs over, the one named last changes fastest.
Arguments:
- weight_query: bfloat16 [12288, 3072], P(('job', 'zero'), 'cols'), parts along dimension 0, may hold values from -0.109375 to 0.109375
- low_query: bfloat16 [12288, 32], P(('job', 'zero')), parts along dimension 0, may hold values from -0.109375 to 0.109375
- high_query: bfloat16 [128, 3072], P('job', 'cols'), parts along dimension 0, may hold values from -1 to 1
- weight_key: bfloat16 [12288, 1024], P(('job', 'zero'), 'cols'), parts along dimension 0, may hold values from -0.109375 to 0.109375
- low_key: bfloat16 [12288, 32], P(('job', 'zero')), parts along dimension 0, may hold values from -0.109375 to 0.109375
- high_key: bfloat16 [128, 1024], P('job', 'cols'), parts along dimension 0, may hold values from -1 to 1
- weight_value: bfloat16 [12288, 1024], P(('job', 'zero'), 'cols'), parts along dimension 0, may hold values from -0.109375 to 0.109375
- low_value: bfloat16 [12288, 32], P(('job', 'zero')), parts along dimension 0, may hold values from -0.109375 to 0.109375
- high_value: bfloat16 [128, 1024], P('job', 'cols'), parts along dimension 0, may hold values from -1 to 1
- weight_mixed: bfloat16 [12288, 3072], P(('job', 'cols'), 'zero'), parts along dimension 0, may hold values from -0.109375 to 0.109375
- low_mixed: bfloat16 [12288, 32], P(('job', 'cols')), parts along dimension 0, may hold values from -0.109375 to 0.109375
- high_mixed: bfloat16 [128, 3072], P('job', 'zero'), parts along dimension 0, may hold values from -1 to 1
- norm_train: float32 [12288], P(('job', 'zero', 'cols')), parts along dimension 0, may hold values from 0.25 to 1.75
- norm_step: float32 [12288], P(('job', 'zero', 'cols')), parts along dimension 0, may hold values from -0.3 to 0.3
Outputs:
- serving_query: bfloat16 [12288, 3072], P('job', 'cols'), parts along dimension 0
- serving_key: bfloat16 [12288, 1024], P('job', 'cols'), parts along dimension 0
- serving_value: bfloat16 [12288, 1024], P('job', 'cols'), parts along dimension 0
- serving_mixed: bfloat16 [12288, 3072], P(('job', 'cols')), parts along dimension 0
- serve_norm: bfloat16 [12288], P('job'), parts along dimension 0
The draws below stay inside these ranges and needn't reach their ends.
There are 4 independent parts, one for each index of `job`. The reference program is written for one: setup_inputs(seed, part) draws one part's arguments, and reference() takes and returns one part's arrays. A program takes and returns all parts, laid end to end along the dimension named above; each array names one. Nothing has to cross between parts.
All inputs are finite; a program needn't handle non-finite values.
Results may differ from the reference program's by a relative error of at most 0.001.
Values may be sent and summed in bfloat16 or wider, within the bound.
A program may use at most 128 MiB of HBM per device.

```python
import jax
import jax.numpy as jnp

D_MODEL = 3072
Q_DIM = 3072
KV_DIM = 1024
RANK = 32


def shard_levels(own_key, extent, split, smallest, high):
    def one(axis_at, shards_of):
        draws = jax.random.uniform(jax.random.fold_in(jax.random.fold_in(own_key, 6), axis_at), (shards_of,), jnp.float32, smallest / len(split), high / len(split))
        return jnp.repeat(jnp.exp(draws), extent[axis_at] // shards_of).reshape((-1,) + (1,) * (len(extent) - axis_at - 1))

    loudness = one(*split[0])
    for cut in split[1:]:
        loudness = loudness * one(*cut)
    return loudness


def bell_draw(stream_key, dims, spread, most, cuts=(), dtype=jnp.bfloat16):
    gain = shard_levels(stream_key, dims, cuts, -0.22, 0.18) if cuts else 1.0
    drawn = jax.random.normal(stream_key, dims, jnp.float32) * spread * gain
    return jnp.minimum(jnp.maximum(drawn, -most), most).astype(dtype)


def setup_inputs(seed: int = 0, part: int = 0) -> dict:
    arg_keys = jax.random.split(jax.random.key(seed), 15)
    own_keys = jax.random.split(jax.random.fold_in(arg_keys[14], part), 15)
    return {
        "weight_query": bell_draw(own_keys[0], (D_MODEL, Q_DIM), D_MODEL ** -0.5, 0.109375, ((0, 16), (1, 4))),
        "low_query": bell_draw(own_keys[1], (D_MODEL, RANK), D_MODEL ** -0.5, 0.109375, ((0, 16),)),
        "high_query": bell_draw(own_keys[2], (RANK, Q_DIM), RANK ** -0.5, 1.0, ((1, 4),)),
        "weight_key": bell_draw(own_keys[3], (D_MODEL, KV_DIM), D_MODEL ** -0.5, 0.109375, ((0, 16), (1, 4))),
        "low_key": bell_draw(own_keys[4], (D_MODEL, RANK), D_MODEL ** -0.5, 0.109375, ((0, 16),)),
        "high_key": bell_draw(own_keys[5], (RANK, KV_DIM), RANK ** -0.5, 1.0, ((1, 4),)),
        "weight_value": bell_draw(own_keys[6], (D_MODEL, KV_DIM), D_MODEL ** -0.5, 0.109375, ((0, 16), (1, 4))),
        "low_value": bell_draw(own_keys[7], (D_MODEL, RANK), D_MODEL ** -0.5, 0.109375, ((0, 16),)),
        "high_value": bell_draw(own_keys[8], (RANK, KV_DIM), RANK ** -0.5, 1.0, ((1, 4),)),
        "weight_mixed": bell_draw(own_keys[9], (Q_DIM, D_MODEL), Q_DIM ** -0.5, 0.109375, ((0, 4), (1, 16))),
        "low_mixed": bell_draw(own_keys[10], (Q_DIM, RANK), Q_DIM ** -0.5, 0.109375, ((0, 4),)),
        "high_mixed": bell_draw(own_keys[11], (RANK, D_MODEL), RANK ** -0.5, 1.0, ((1, 16),)),
        "norm_train": jnp.clip(1.0 + 0.15 * jax.random.normal(own_keys[12], (D_MODEL,), jnp.float32), 0.25, 1.75),
        "norm_step": jnp.clip(jax.random.uniform(own_keys[13], (D_MODEL,), jnp.float32, -0.3, 0.3) * shard_levels(own_keys[13], (D_MODEL,), ((0, 64),), -0.4, 0.0), -0.3, 0.3),
    }


mix_rate = 2.0


def reference(weight_query, low_query, high_query, weight_key, low_key, high_key, weight_value, low_value, high_value, weight_mixed, low_mixed, high_mixed, norm_train, norm_step):
    whole_query = weight_query.astype(jnp.float32) + mix_rate * jnp.dot(low_query, high_query, preferred_element_type=jnp.float32)
    whole_key = weight_key.astype(jnp.float32) + mix_rate * jnp.dot(low_key, high_key, preferred_element_type=jnp.float32)
    whole_value = weight_value.astype(jnp.float32) + mix_rate * jnp.dot(low_value, high_value, preferred_element_type=jnp.float32)
    whole_mixed = weight_mixed.astype(jnp.float32) + mix_rate * jnp.dot(low_mixed, high_mixed, preferred_element_type=jnp.float32)
    serving_query = whole_query.astype(jnp.bfloat16)
    serving_key = whole_key.astype(jnp.bfloat16)
    serving_value = whole_value.astype(jnp.bfloat16)
    serving_mixed = whole_mixed.astype(jnp.bfloat16)
    serve_norm = (norm_train + norm_step).astype(jnp.bfloat16)
    return serving_query, serving_key, serving_value, serving_mixed, serve_norm
```

```python
import functools

import jax
import jax.numpy as jnp
from jax import lax
from jax.experimental import pallas as pl
from jax.experimental.pallas import tpu as pltpu
from jax.sharding import PartitionSpec as P

mix_rate = 2.0
MESH = pl.DeviceIdType.MESH
BF16 = jnp.bfloat16
F32 = jnp.float32

PIECES = ("q0", "q1", "norm", "q2", "k", "v", "m0", "m1", "m2")
UP = {"q0": 4, "q1": 4, "norm": 4, "q2": 4, "k": 4, "v": 3, "m0": 3, "m1": 3, "m2": 3}


def merged(base, low_turned, high):
    delta = lax.dot_general(
        low_turned, high, (((0,), (0,)), ((), ())), preferred_element_type=F32
    )
    return (base.astype(F32) + mix_rate * delta).astype(BF16)


def gather_kernel(
    wq, lq, hq, wk, lk, hk, wv, lv, hv, wm, lm, hm, nt, ns,
    q_all, k_all, v_all, m_all, n_out,
    wq_v, lq_v, hq_v, wk_v, lk_v, hk_v, wv_v, lv_v, hv_v, wm_v, lm_v, hm_v, nt_v, ns_v,
    n_all, n_wide,
    load_sem, pair_sem, side_sem, own_sem, send_sem, recv_sem, hand_sem, take_sem,
):
    zero = lax.axis_index("zero")
    col = lax.axis_index("cols")
    core = lax.rem(zero, 2)
    chip = lax.div(zero, 2)
    above = lax.rem(zero + 2, 16)
    below = lax.rem(zero + 14, 16)
    twin = zero + 1 - 2 * core

    barrier = pltpu.get_barrier_semaphore()
    for peer in (above, below, twin):
        pl.semaphore_signal(
            barrier, inc=1, device_id={"zero": peer}, device_id_type=MESH
        )
    for far in (1, 2, 3):
        pl.semaphore_signal(
            barrier,
            inc=1,
            device_id={"cols": lax.rem(col + far, 4)},
            device_id_type=MESH,
        )

    half = pl.ds(pl.multiple_of(384 * core, 128), 384)
    other_half = pl.ds(pl.multiple_of(384 * (1 - core), 128), 384)
    my_rows = pl.ds(pl.multiple_of(192 * core, 64), 192)
    loads = [
        pltpu.make_async_copy(src, dst, load_sem.at[i])
        for i, (src, dst) in enumerate(
            (
                (lq, lq_v),
                (hq, hq_v),
                (wq, wq_v),
                (nt, nt_v),
                (ns, ns_v),
                (lk, lk_v),
                (hk, hk_v),
                (wk, wk_v),
                (lv, lv_v),
                (hv, hv_v),
                (wv, wv_v),
                (hm, hm_v.at[core]),
                (wm.at[:, half], wm_v.at[my_rows]),
                (lm.at[:, half], lm_v),
            )
        )
    ]
    for load in loads:
        load.start()

    def place(name, origin):
        rows = 192 * (2 * origin + core)
        if name == "norm":
            return n_all.at[2 * origin + core]
        if name == "k":
            return k_all.at[pl.ds(pl.multiple_of(rows, 64), 192)]
        if name == "v":
            return v_all.at[pl.ds(pl.multiple_of(rows, 64), 192)]
        i = int(name[1])
        if name[0] == "q":
            return q_all.at[pl.ds(pl.multiple_of(rows + 64 * i, 64), 64)]
        return m_all.at[origin, pl.ds(pl.multiple_of(384 * core + 128 * i, 128), 128)]

    def ring_copy(name, way, step):
        i = PIECES.index(name)
        origin = lax.rem(chip + (8 - step if way == 0 else step), 8)
        piece = place(name, origin)
        return pltpu.make_async_remote_copy(
            src_ref=piece,
            dst_ref=piece,
            send_sem=send_sem.at[way, step, i],
            recv_sem=recv_sem.at[way, step, i],
            device_id={"zero": above if way == 0 else below},
            device_id_type=MESH,
        )

    def arrival(name, way, step):
        i = PIECES.index(name)
        origin = lax.rem(chip + (7 - step if way == 0 else step + 1), 8)
        piece = place(name, origin)
        return pltpu.make_async_remote_copy(
            src_ref=piece,
            dst_ref=piece,
            send_sem=send_sem.at[way, step, i],
            recv_sem=recv_sem.at[way, step, i],
            device_id={"zero": below if way == 0 else above},
            device_id_type=MESH,
        )

    def twin_place(name, origin):
        rows = 192 * (2 * origin + 1 - core)
        if name == "norm":
            return n_all.at[2 * origin + 1 - core]
        if name == "k":
            return k_all.at[pl.ds(pl.multiple_of(rows, 64), 192)]
        if name == "v":
            return v_all.at[pl.ds(pl.multiple_of(rows, 64), 192)]
        i = int(name[1])
        if name[0] == "q":
            return q_all.at[pl.ds(pl.multiple_of(rows + 64 * i, 64), 64)]
        return m_all.at[
            origin, pl.ds(pl.multiple_of(384 * (1 - core) + 128 * i, 128), 128)
        ]

    def hand(name, way, step):
        i = PIECES.index(name)
        if step < 0:
            origin = chip
        else:
            origin = lax.rem(chip + (7 - step if way == 0 else step + 1), 8)
        slot = step + 1
        mine = place(name, origin)
        return pltpu.make_async_remote_copy(
            src_ref=mine,
            dst_ref=mine,
            send_sem=hand_sem.at[way, slot, i],
            recv_sem=take_sem.at[way, slot, i],
            device_id={"zero": twin},
            device_id_type=MESH,
        )

    def take(name, way, step):
        i = PIECES.index(name)
        if step < 0:
            origin = chip
        else:
            origin = lax.rem(chip + (7 - step if way == 0 else step + 1), 8)
        slot = step + 1
        theirs = twin_place(name, origin)
        return pltpu.make_async_remote_copy(
            src_ref=theirs,
            dst_ref=theirs,
            send_sem=hand_sem.at[way, slot, i],
            recv_sem=take_sem.at[way, slot, i],
            device_id={"zero": twin},
            device_id_type=MESH,
        )

    def hops(name, way):
        return UP[name] if way == 0 else 7 - UP[name]

    sends, hands, takes = [], [], []

    def send(name, way, step):
        copy = ring_copy(name, way, step)
        copy.start()
        sends.append(copy)

    def give(name, way, step):
        copy = hand(name, way, step)
        copy.start()
        hands.append(copy)
        takes.append((name, way, step))

    def launch(name):
        send(name, 0, 0)
        send(name, 1, 0)
        give(name, 0, -1)

    for i in (0, 1, 2):
        loads[i].wait()
    own = 192 * zero
    q_all[pl.ds(pl.multiple_of(own, 64), 192), :] = merged(
        wq_v[...], lq_v[...], hq_v[...]
    )
    loads[3].wait()
    loads[4].wait()
    n_all[zero, col] = jnp.zeros((1, 128), F32)
    n_all[zero, col, :, 0:48] = nt_v[...] + ns_v[...]

    pl.semaphore_wait(barrier, 6)
    launch("q0")
    launch("q1")
    sides = []
    for far in (1, 2, 3):
        copy = pltpu.make_async_remote_copy(
            src_ref=n_all.at[zero, col],
            dst_ref=n_all.at[zero, col],
            send_sem=side_sem.at[0, far - 1],
            recv_sem=side_sem.at[1, far - 1],
            device_id={"cols": lax.rem(col + far, 4)},
            device_id_type=MESH,
        )
        copy.start()
        sides.append(copy)
    pair = [
        pltpu.make_async_remote_copy(
            src_ref=src,
            dst_ref=dst,
            send_sem=pair_sem.at[0, i],
            recv_sem=pair_sem.at[1, i],
            device_id={"zero": twin},
            device_id_type=MESH,
        )
        for i, (src, dst) in enumerate(
            ((wm.at[:, other_half], wm_v.at[my_rows]), (hm, hm_v.at[core]))
        )
    ]
    for copy in pair:
        copy.start()

    for i in (5, 6, 7):
        loads[i].wait()
    k_all[pl.ds(pl.multiple_of(own, 64), 192), :] = merged(
        wk_v[...], lk_v[...], hk_v[...]
    )
    for i in (8, 9, 10):
        loads[i].wait()
    v_all[pl.ds(pl.multiple_of(own, 64), 192), :] = merged(
        wv_v[...], lv_v[...], hv_v[...]
    )
    for far in (1, 2, 3):
        src = lax.rem(col + 4 - far, 4)
        pltpu.make_async_remote_copy(
            src_ref=n_all.at[zero, src],
            dst_ref=n_all.at[zero, src],
            send_sem=side_sem.at[0, far - 1],
            recv_sem=side_sem.at[1, far - 1],
            device_id={"cols": src},
            device_id_type=MESH,
        ).wait_recv()
    launch("norm")
    launch("q2")
    launch("k")
    launch("v")

    for i in (11, 12, 13):
        loads[i].wait()
    twin_rows = pl.ds(pl.multiple_of(192 * (1 - core), 64), 192)
    for i, dst in enumerate((wm_v.at[twin_rows], hm_v.at[1 - core])):
        pltpu.make_async_remote_copy(
            src_ref=dst,
            dst_ref=dst,
            send_sem=pair_sem.at[0, i],
            recv_sem=pair_sem.at[1, i],
            device_id={"zero": twin},
            device_id_type=MESH,
        ).wait_recv()
    row = lax.broadcasted_iota(jnp.int32, (192, 384), 0)
    lane = lax.broadcasted_iota(jnp.int32, (192, 384), 1)
    high = sum(
        jnp.dot(
            hm_v[c], (lane == row + 192 * c).astype(BF16), preferred_element_type=F32
        )
        for c in (0, 1)
    ).astype(BF16)
    for i in (0, 1, 2):
        lanes = slice(128 * i, 128 * i + 128)
        base = wm_v[:, lanes].astype(F32).T
        m_all[chip, pl.ds(pl.multiple_of(384 * core + 128 * i, 128), 128)] = merged(
            base, lm_v[:, lanes], high
        )
        launch(f"m{i}")
    for copy in sides + pair:
        copy.wait_send()

    def norm_out():
        for name, way, step in [t for t in takes if t[0] == "norm"]:
            take(name, way, step).wait_recv()
            takes.remove((name, way, step))
        at = lax.broadcasted_iota(jnp.int32, (1, 128), 1)
        for g in range(8):
            e = [n_all[2 * g + i // 4, i % 4] for i in range(8)]
            r = [pltpu.roll(e[i], (48 * i) % 128, 1) for i in range(8)]
            n_wide[3 * g : 3 * g + 1, :] = jnp.where(
                at < 48, r[0], jnp.where(at < 96, r[1], r[2])
            )
            n_wide[3 * g + 1 : 3 * g + 2, :] = jnp.where(
                at < 16,
                r[2],
                jnp.where(at < 64, r[3], jnp.where(at < 112, r[4], r[5])),
            )
            n_wide[3 * g + 2 : 3 * g + 3, :] = jnp.where(
                at < 32, r[5], jnp.where(at < 80, r[6], r[7])
            )
        n_out[...] = n_wide[...].astype(BF16)

    for step in range(4):
        todo = [
            [name for name in PIECES if step < hops(name, way)] for way in (0, 1)
        ]
        for n in range(max(map(len, todo))):
            if step == 3 and n == 4:
                norm_out()
                for copy in sends + hands:
                    copy.wait_send()
                del sends[:], hands[:]
            for way in (0, 1):
                if n < len(todo[way]):
                    name = todo[way][n]
                    arrival(name, way, step).wait_recv()
                    if step + 1 < hops(name, way):
                        send(name, way, step + 1)
                    give(name, way, step)
    for copy in sends + hands:
        copy.wait_send()
    for name, way, step in takes:
        take(name, way, step).wait_recv()


def store_kernel(q, k, v, m, n, q_out, k_out, v_out, m_out, n_out, sem):
    parts = [
        (q.at[pl.ds(768 * i, 768)], q_out.at[pl.ds(768 * i, 768)]) for i in range(4)
    ]
    parts += [(k, k_out), (v, v_out), (n, n_out)]
    parts += [(m.at[i], m_out.at[:, pl.ds(384 * i, 384)]) for i in range(8)]
    copies = [
        pltpu.make_async_copy(src, dst, sem.at[i]) for i, (src, dst) in enumerate(parts)
    ]
    for copy in copies:
        copy.start()
    for copy in copies:
        copy.wait()


def on_device(wq, lq, hq, wk, lk, hk, wv, lv, hv, wm, lm, hm, nt, ns):
    anywhere = pl.BlockSpec(memory_space=pltpu.HBM)
    onchip = pl.BlockSpec(memory_space=pltpu.VMEM)
    n = len(PIECES)
    held = pl.pallas_call(
        gather_kernel,
        out_shape=(
            pltpu.VMEM((3072, 768), BF16),
            pltpu.VMEM((3072, 256), BF16),
            pltpu.VMEM((3072, 256), BF16),
            pltpu.VMEM((8, 768, 384), BF16),
            pltpu.VMEM((24, 128), BF16),
        ),
        in_specs=[anywhere] * 14,
        out_specs=(onchip,) * 5,
        scratch_shapes=[
            pltpu.VMEM((192, 768), BF16),
            pltpu.VMEM((32, 192), BF16),
            pltpu.VMEM((32, 768), BF16),
            pltpu.VMEM((192, 256), BF16),
            pltpu.VMEM((32, 192), BF16),
            pltpu.VMEM((32, 256), BF16),
            pltpu.VMEM((192, 256), BF16),
            pltpu.VMEM((32, 192), BF16),
            pltpu.VMEM((32, 256), BF16),
            pltpu.VMEM((384, 384), BF16),
            pltpu.VMEM((32, 384), BF16),
            pltpu.VMEM((2, 32, 192), BF16),
            pltpu.VMEM((1, 48), F32),
            pltpu.VMEM((1, 48), F32),
            pltpu.VMEM((16, 4, 1, 128), F32),
            pltpu.VMEM((24, 128), F32),
            pltpu.SemaphoreType.DMA((14,)),
            pltpu.SemaphoreType.DMA((2, 2)),
            pltpu.SemaphoreType.DMA((2, 3)),
            pltpu.SemaphoreType.DMA,
            pltpu.SemaphoreType.DMA((2, 4, n)),
            pltpu.SemaphoreType.DMA((2, 4, n)),
            pltpu.SemaphoreType.DMA((2, 5, n)),
            pltpu.SemaphoreType.DMA((2, 5, n)),
        ],
        compiler_params=pltpu.CompilerParams(
            collective_id=0, has_side_effects=True, vmem_limit_bytes=54400000
        ),
        name="merge_and_gather",
    )(
        wq, lq.T, hq, wk, lk.T, hk, wv, lv.T, hv, wm.T, lm.T, hm,
        nt.reshape(1, 48), ns.reshape(1, 48),
    )
    q, k, v, m, norm = pl.pallas_call(
        store_kernel,
        out_shape=(
            jax.ShapeDtypeStruct((3072, 768), BF16),
            jax.ShapeDtypeStruct((3072, 256), BF16),
            jax.ShapeDtypeStruct((3072, 256), BF16),
            jax.ShapeDtypeStruct((768, 3072), BF16),
            jax.ShapeDtypeStruct((24, 128), BF16),
        ),
        in_specs=[onchip] * 5,
        out_specs=(anywhere,) * 5,
        scratch_shapes=[pltpu.SemaphoreType.DMA((15,))],
        compiler_params=pltpu.CompilerParams(vmem_limit_bytes=24 * 2**20),
        name="store",
    )(*held)
    return q, k, v, m, norm.reshape(3072)


def solution(mesh):
    placed = (
        P(("job", "zero"), "cols"),
        P(("job", "zero"), None),
        P("job", "cols"),
        P(("job", "zero"), "cols"),
        P(("job", "zero"), None),
        P("job", "cols"),
        P(("job", "zero"), "cols"),
        P(("job", "zero"), None),
        P("job", "cols"),
        P(("job", "cols"), "zero"),
        P(("job", "cols"), None),
        P("job", "zero"),
        P(("job", "zero", "cols")),
        P(("job", "zero", "cols")),
    )
    return jax.shard_map(
        on_device,
        mesh=mesh,
        in_specs=placed,
        out_specs=(
            P("job", "cols"),
            P("job", "cols"),
            P("job", "cols"),
            P(("job", "cols"), None),
            P("job"),
        ),
        check_vma=False,
    )
```

```python
import functools

import jax
import jax.numpy as jnp
from jax import lax
from jax.experimental import pallas as pl
from jax.experimental.pallas import tpu as pltpu
from jax.sharding import PartitionSpec as P

mix_rate = 2.0
MESH = pl.DeviceIdType.MESH
BF16 = jnp.bfloat16
F32 = jnp.float32

PIECES = ("k", "v", "q", "norm", "m")
ORDER = (("k", "v", "q", "norm", "m"), ("k", "q", "norm", "m", "v"))
LAST = (("q", "norm", "v"), ("m", "k"))
UP = {"q": 4, "v": 4, "norm": 4, "k": 3, "m": 3}
KIND = {"q": 0, "k": 0, "v": 1, "m": 1, "norm": 2}
SIZE = {"q": 288, "k": 96, "v": 96, "m": 288, "norm": 2}


def by_arrival(orders):
    timed = []
    for way, order in enumerate(orders):
        at = 0
        for name in order:
            at += SIZE[name]
            timed.append((at, way, name))
    return [(name, way) for _, way, name in sorted(timed)]


def merged(base, low_turned, high):
    delta = lax.dot_general(
        low_turned, high, (((0,), (0,)), ((), ())), preferred_element_type=F32
    )
    return (base.astype(F32) + mix_rate * delta).astype(BF16)


def gather_kernel(
    wq, lq, hq, wk, lk, hk, wv, lv, hv, wm, lm, hm, nt, ns,
    q_all, k_all, v_all, m_all, n_out,
    wq_v, lq_v, hq_v, wk_v, lk_v, hk_v, wv_v, lv_v, hv_v, wm_v, lm_v, hm_v, nt_v, ns_v,
    n_all, n_wide,
    load_sem, pair_sem, side_sem, send_sem, recv_sem, hand_sem, take_sem,
):
    zero = lax.axis_index("zero")
    col = lax.axis_index("cols")
    core = lax.rem(zero, 2)
    chip = lax.div(zero, 2)
    above = lax.rem(zero + 2, 16)
    below = lax.rem(zero + 14, 16)
    twin = zero + 1 - 2 * core

    barrier = pltpu.get_barrier_semaphore()
    for peer in (above, below, twin):
        pl.semaphore_signal(
            barrier, inc=1, device_id={"zero": peer}, device_id_type=MESH
        )
    for far in (1, 2, 3):
        pl.semaphore_signal(
            barrier,
            inc=1,
            device_id={"cols": lax.rem(col + far, 4)},
            device_id_type=MESH,
        )

    half = pl.ds(pl.multiple_of(384 * core, 128), 384)
    other_half = pl.ds(pl.multiple_of(384 * (1 - core), 128), 384)
    my_rows = pl.ds(pl.multiple_of(192 * core, 64), 192)
    loads = [
        pltpu.make_async_copy(src, dst, load_sem.at[i])
        for i, (src, dst) in enumerate(
            (
                (lk, lk_v),
                (hk, hk_v),
                (wk, wk_v),
                (lv, lv_v),
                (hv, hv_v),
                (wv, wv_v),
                (lq, lq_v),
                (hq, hq_v),
                (wq, wq_v),
                (nt, nt_v),
                (ns, ns_v),
                (hm, hm_v.at[core]),
                (wm.at[:, half], wm_v.at[my_rows]),
                (lm.at[:, half], lm_v),
            )
        )
    ]
    for load in loads:
        load.start()

    def place(name, origin, of):
        if name == "norm":
            return n_all.at[2 * origin + of]
        if name == "m":
            return m_all.at[origin, pl.ds(pl.multiple_of(384 * of, 128), 384)]
        rows = pl.ds(pl.multiple_of(192 * (2 * origin + of), 64), 192)
        return {"q": q_all, "k": k_all, "v": v_all}[name].at[rows]

    arrivals = [
        (name, way, step)
        for way in (0, 1)
        for name in PIECES
        for step in range(UP[name] if way == 0 else 7 - UP[name])
    ]

    def arrived_from(way, step):
        return lax.rem(chip + (7 - step if way == 0 else step + 1), 8)

    def ring_copy(name, way, step):
        origin = lax.rem(chip + (8 - step if way == 0 else step), 8)
        piece = place(name, origin, core)
        return pltpu.make_async_remote_copy(
            src_ref=piece,
            dst_ref=piece,
            send_sem=send_sem.at[2 if name == "norm" else way],
            recv_sem=recv_sem.at[arrivals.index((name, way, step))],
            device_id={"zero": above if way == 0 else below},
            device_id_type=MESH,
        )

    def arrival(name, way, step):
        piece = place(name, arrived_from(way, step), core)
        return pltpu.make_async_remote_copy(
            src_ref=piece,
            dst_ref=piece,
            send_sem=send_sem.at[2 if name == "norm" else way],
            recv_sem=recv_sem.at[arrivals.index((name, way, step))],
            device_id={"zero": below if way == 0 else above},
            device_id_type=MESH,
        )

    def give(name, way, step):
        origin = chip if step < 0 else arrived_from(way, step)
        piece = place(name, origin, core)
        pltpu.make_async_remote_copy(
            src_ref=piece,
            dst_ref=piece,
            send_sem=hand_sem.at[KIND[name]],
            recv_sem=take_sem.at[KIND[name]],
            device_id={"zero": twin},
            device_id_type=MESH,
        ).start()

    def send(name, way, step):
        ring_copy(name, way, step).start()

    def drain(sem, *refs):
        for ref in refs:
            pltpu.make_async_copy(ref, ref, sem).wait()

    own = pl.ds(pl.multiple_of(192 * zero, 64), 192)
    for i in (0, 1, 2):
        loads[i].wait()
    k_all[own, :] = merged(wk_v[...], lk_v[...], hk_v[...])
    pl.semaphore_wait(barrier, 6)
    send("k", 0, 0)
    send("k", 1, 0)
    for i in (3, 4, 5):
        loads[i].wait()
    v_all[own, :] = merged(wv_v[...], lv_v[...], hv_v[...])
    send("v", 0, 0)
    for i in (6, 7, 8):
        loads[i].wait()
    q_all[own, :] = merged(wq_v[...], lq_v[...], hq_v[...])
    send("q", 0, 0)
    send("q", 1, 0)

    loads[9].wait()
    loads[10].wait()
    n_all[zero, col] = jnp.zeros((1, 128), F32)
    n_all[zero, col, :, 0:48] = nt_v[...] + ns_v[...]
    pair = [
        pltpu.make_async_remote_copy(
            src_ref=src,
            dst_ref=dst,
            send_sem=pair_sem.at[0, i],
            recv_sem=pair_sem.at[1, i],
            device_id={"zero": twin},
            device_id_type=MESH,
        )
        for i, (src, dst) in enumerate(
            ((wm.at[:, other_half], wm_v.at[my_rows]), (hm, hm_v.at[core]))
        )
    ]
    for copy in pair:
        copy.start()
    sides = []
    for far in (1, 2, 3):
        copy = pltpu.make_async_remote_copy(
            src_ref=n_all.at[zero, col],
            dst_ref=n_all.at[zero, col],
            send_sem=side_sem.at[0, far - 1],
            recv_sem=side_sem.at[1, far - 1],
            device_id={"cols": lax.rem(col + far, 4)},
            device_id_type=MESH,
        )
        copy.start()
        sides.append(copy)
    for name in ("k", "v", "q"):
        give(name, 0, -1)

    for i in (11, 12, 13):
        loads[i].wait()
    twin_rows = pl.ds(pl.multiple_of(192 * (1 - core), 64), 192)
    for i, dst in enumerate((wm_v.at[twin_rows], hm_v.at[1 - core])):
        pltpu.make_async_remote_copy(
            src_ref=dst,
            dst_ref=dst,
            send_sem=pair_sem.at[0, i],
            recv_sem=pair_sem.at[1, i],
            device_id={"zero": twin},
            device_id_type=MESH,
        ).wait_recv()
    row = lax.broadcasted_iota(jnp.int32, (192, 384), 0)
    lane = lax.broadcasted_iota(jnp.int32, (192, 384), 1)
    high = sum(
        jnp.dot(
            hm_v[c], (lane == row + 192 * c).astype(BF16), preferred_element_type=F32
        )
        for c in (0, 1)
    ).astype(BF16)
    for i in (0, 1, 2):
        lanes = slice(128 * i, 128 * i + 128)
        base = wm_v[:, lanes].astype(F32).T
        m_all[chip, pl.ds(pl.multiple_of(384 * core + 128 * i, 128), 128)] = merged(
            base, lm_v[:, lanes], high
        )
    for far in (1, 2, 3):
        src = lax.rem(col + 4 - far, 4)
        pltpu.make_async_remote_copy(
            src_ref=n_all.at[zero, src],
            dst_ref=n_all.at[zero, src],
            send_sem=side_sem.at[0, far - 1],
            recv_sem=side_sem.at[1, far - 1],
            device_id={"cols": src},
            device_id_type=MESH,
        ).wait_recv()
    send("norm", 0, 0)
    send("norm", 1, 0)
    send("m", 0, 0)
    send("m", 1, 0)
    send("v", 1, 0)
    give("norm", 0, -1)
    give("m", 0, -1)
    for copy in sides + pair:
        copy.wait_send()

    def norm_out():
        drain(take_sem.at[2], n_all.at[0:8])
        at = lax.broadcasted_iota(jnp.int32, (1, 128), 1)
        for g in range(8):
            e = [n_all[2 * g + i // 4, i % 4] for i in range(8)]
            r = [pltpu.roll(e[i], (48 * i) % 128, 1) for i in range(8)]
            n_wide[3 * g : 3 * g + 1, :] = jnp.where(
                at < 48, r[0], jnp.where(at < 96, r[1], r[2])
            )
            n_wide[3 * g + 1 : 3 * g + 2, :] = jnp.where(
                at < 16,
                r[2],
                jnp.where(at < 64, r[3], jnp.where(at < 112, r[4], r[5])),
            )
            n_wide[3 * g + 2 : 3 * g + 3, :] = jnp.where(
                at < 32, r[5], jnp.where(at < 80, r[6], r[7])
            )
        n_out[...] = n_wide[...].astype(BF16)

    for step in range(3):
        for name, way in by_arrival(ORDER):
            arrival(name, way, step).wait_recv()
            if step < 2:
                send(name, way, step + 1)
            elif name == LAST[way][-2]:
                send(name, way, 3)
                send(LAST[way][-1], way, 3)
            elif name in LAST[way][:-2]:
                send(name, way, 3)
            give(name, way, step)
    last = by_arrival(LAST)
    for name, way in last[:-2]:
        arrival(name, way, 3).wait_recv()
        give(name, way, 3)
    norm_out()
    for name, way in last[-2:]:
        arrival(name, way, 3).wait_recv()
        give(name, way, 3)
    for way in (0, 1):
        drain(send_sem.at[way], q_all.at[0:1792])
    drain(send_sem.at[2], n_all.at[0:7])
    drain(hand_sem.at[2], n_all.at[0:8])
    for kind in (0, 1):
        drain(hand_sem.at[kind], q_all.at[0:2048])
        drain(take_sem.at[kind], q_all.at[0:2048])


def store_kernel(q, k, v, m, n, q_out, k_out, v_out, m_out, n_out, sem):
    parts = [
        (q.at[pl.ds(768 * i, 768)], q_out.at[pl.ds(768 * i, 768)], 0) for i in range(4)
    ]
    parts += [(m.at[i], m_out.at[:, pl.ds(384 * i, 384)], 1) for i in range(8)]
    parts += [(k, k_out, 2), (v, v_out, 3), (n, n_out, 4)]
    for src, dst, i in parts:
        pltpu.make_async_copy(src, dst, sem.at[i]).start()
    for i, (src, dst) in enumerate(
        ((q, q_out), (m_out, m_out), (k, k_out), (v, v_out), (n, n_out))
    ):
        pltpu.make_async_copy(src, dst, sem.at[i]).wait()


def on_device(wq, lq, hq, wk, lk, hk, wv, lv, hv, wm, lm, hm, nt, ns):
    anywhere = pl.BlockSpec(memory_space=pltpu.HBM)
    onchip = pl.BlockSpec(memory_space=pltpu.VMEM)
    held = pl.pallas_call(
        gather_kernel,
        out_shape=(
            pltpu.VMEM((3072, 768), BF16),
            pltpu.VMEM((3072, 256), BF16),
            pltpu.VMEM((3072, 256), BF16),
            pltpu.VMEM((8, 768, 384), BF16),
            pltpu.VMEM((24, 128), BF16),
        ),
        in_specs=[anywhere] * 14,
        out_specs=(onchip,) * 5,
        scratch_shapes=[
            pltpu.VMEM((192, 768), BF16),
            pltpu.VMEM((32, 192), BF16),
            pltpu.VMEM((32, 768), BF16),
            pltpu.VMEM((192, 256), BF16),
            pltpu.VMEM((32, 192), BF16),
            pltpu.VMEM((32, 256), BF16),
            pltpu.VMEM((192, 256), BF16),
            pltpu.VMEM((32, 192), BF16),
            pltpu.VMEM((32, 256), BF16),
            pltpu.VMEM((384, 384), BF16),
            pltpu.VMEM((32, 384), BF16),
            pltpu.VMEM((2, 32, 192), BF16),
            pltpu.VMEM((1, 48), F32),
            pltpu.VMEM((1, 48), F32),
            pltpu.VMEM((16, 4, 1, 128), F32),
            pltpu.VMEM((24, 128), F32),
            pltpu.SemaphoreType.DMA((14,)),
            pltpu.SemaphoreType.DMA((2, 2)),
            pltpu.SemaphoreType.DMA((2, 3)),
            pltpu.SemaphoreType.DMA((3,)),
            pltpu.SemaphoreType.DMA((7 * len(PIECES),)),
            pltpu.SemaphoreType.DMA((3,)),
            pltpu.SemaphoreType.DMA((3,)),
        ],
        compiler_params=pltpu.CompilerParams(
            collective_id=0, has_side_effects=True, vmem_limit_bytes=54400000
        ),
        name="merge_and_gather",
    )(
        wq, lq.T, hq, wk, lk.T, hk, wv, lv.T, hv, wm.T, lm.T, hm,
        nt.reshape(1, 48), ns.reshape(1, 48),
    )
    q, k, v, m, norm = pl.pallas_call(
        store_kernel,
        out_shape=(
            jax.ShapeDtypeStruct((3072, 768), BF16),
            jax.ShapeDtypeStruct((3072, 256), BF16),
            jax.ShapeDtypeStruct((3072, 256), BF16),
            jax.ShapeDtypeStruct((768, 3072), BF16),
            jax.ShapeDtypeStruct((24, 128), BF16),
        ),
        in_specs=[onchip] * 5,
        out_specs=(anywhere,) * 5,
        scratch_shapes=[pltpu.SemaphoreType.DMA((5,))],
        compiler_params=pltpu.CompilerParams(vmem_limit_bytes=24 * 2**20),
        name="store",
    )(*held)
    return q, k, v, m, norm.reshape(3072)


def solution(mesh):
    placed = (
        P(("job", "zero"), "cols"),
        P(("job", "zero"), None),
        P("job", "cols"),
        P(("job", "zero"), "cols"),
        P(("job", "zero"), None),
        P("job", "cols"),
        P(("job", "zero"), "cols"),
        P(("job", "zero"), None),
        P("job", "cols"),
        P(("job", "cols"), "zero"),
        P(("job", "cols"), None),
        P("job", "zero"),
        P(("job", "zero", "cols")),
        P(("job", "zero", "cols")),
    )
    return jax.shard_map(
        on_device,
        mesh=mesh,
        in_specs=placed,
        out_specs=(
            P("job", "cols"),
            P("job", "cols"),
            P("job", "cols"),
            P(("job", "cols"), None),
            P("job"),
        ),
        check_vma=False,
    )
```

```python
import functools

import jax
import jax.numpy as jnp
from jax import lax
from jax.experimental import pallas as pl
from jax.experimental.pallas import tpu as pltpu
from jax.sharding import PartitionSpec as P

mix_rate = 2.0
MESH = pl.DeviceIdType.MESH
BF16 = jnp.bfloat16
F32 = jnp.float32

PIECES = ("k", "v", "q", "m")
ORDER = (("k", "v", "q", "m"), ("k", "q", "m", "v"))
LAST = (("q", "v"), ("m", "k"))
UP = {"q": 4, "v": 4, "k": 3, "m": 3}
KIND = {"q": 0, "k": 0, "v": 1, "m": 1}
SIZE = {"q": 288, "k": 96, "v": 96, "m": 288}


def by_arrival(orders):
    timed = []
    for way, order in enumerate(orders):
        at = 0
        for name in order:
            at += SIZE[name]
            timed.append((at, way, name))
    return [(name, way) for _, way, name in sorted(timed)]


def merged(base, low_turned, high):
    delta = lax.dot_general(
        low_turned, high, (((0,), (0,)), ((), ())), preferred_element_type=F32
    )
    return (base.astype(F32) + mix_rate * delta).astype(BF16)


def gather_kernel(
    wq, lq, hq, wk, lk, hk, wv, lv, hv, wm, lm, hm, nt, ns,
    q_all, k_all, v_all, m_all, n_out,
    wq_v, lq_v, hq_v, wk_v, lk_v, hk_v, wv_v, lv_v, hv_v, wm_v, lm_v, hm_v, nt_v, ns_v,
    n_all, n_wide,
    load_sem, pair_sem, send_sem, recv_sem, hand_sem, take_sem, norm_sem,
):
    zero = lax.axis_index("zero")
    col = lax.axis_index("cols")
    core = lax.rem(zero, 2)
    chip = lax.div(zero, 2)
    above = lax.rem(zero + 2, 16)
    below = lax.rem(zero + 14, 16)
    twin = zero + 1 - 2 * core

    barrier = pltpu.get_barrier_semaphore()
    for peer in (above, below, twin):
        pl.semaphore_signal(
            barrier, inc=1, device_id={"zero": peer}, device_id_type=MESH
        )
    is_root = zero == 0

    @pl.when(is_root)
    def _():
        for other in range(1, 16):
            pl.semaphore_signal(
                barrier, inc=1, device_id={"zero": other}, device_id_type=MESH
            )
        for far in (1, 2, 3):
            pl.semaphore_signal(
                barrier,
                inc=1,
                device_id={"cols": lax.rem(col + far, 4)},
                device_id_type=MESH,
            )

    half = pl.ds(pl.multiple_of(384 * core, 128), 384)
    other_half = pl.ds(pl.multiple_of(384 * (1 - core), 128), 384)
    my_rows = pl.ds(pl.multiple_of(192 * core, 64), 192)
    loads = [
        pltpu.make_async_copy(src, dst, load_sem.at[i])
        for i, (src, dst) in enumerate(
            (
                (lk, lk_v),
                (hk, hk_v),
                (wk, wk_v),
                (nt, nt_v),
                (ns, ns_v),
                (lv, lv_v),
                (hv, hv_v),
                (wv, wv_v),
                (lq, lq_v),
                (hq, hq_v),
                (wq, wq_v),
                (hm, hm_v.at[core]),
                (wm.at[:, half], wm_v.at[my_rows]),
                (lm.at[:, half], lm_v),
            )
        )
    ]
    for load in loads:
        load.start()

    def place(name, origin, of):
        if name == "m":
            return m_all.at[origin, pl.ds(pl.multiple_of(384 * of, 128), 384)]
        rows = pl.ds(pl.multiple_of(192 * (2 * origin + of), 64), 192)
        return {"q": q_all, "k": k_all, "v": v_all}[name].at[rows]

    arrivals = [
        (name, way, step)
        for way in (0, 1)
        for name in PIECES
        for step in range(UP[name] if way == 0 else 7 - UP[name])
    ]

    def arrived_from(way, step):
        return lax.rem(chip + (7 - step if way == 0 else step + 1), 8)

    def ring_copy(name, way, step):
        origin = lax.rem(chip + (8 - step if way == 0 else step), 8)
        piece = place(name, origin, core)
        return pltpu.make_async_remote_copy(
            src_ref=piece,
            dst_ref=piece,
            send_sem=send_sem.at[way],
            recv_sem=recv_sem.at[arrivals.index((name, way, step))],
            device_id={"zero": above if way == 0 else below},
            device_id_type=MESH,
        )

    def arrival(name, way, step):
        piece = place(name, arrived_from(way, step), core)
        return pltpu.make_async_remote_copy(
            src_ref=piece,
            dst_ref=piece,
            send_sem=send_sem.at[way],
            recv_sem=recv_sem.at[arrivals.index((name, way, step))],
            device_id={"zero": below if way == 0 else above},
            device_id_type=MESH,
        )

    def give(name, way, step):
        origin = chip if step < 0 else arrived_from(way, step)
        piece = place(name, origin, core)
        pltpu.make_async_remote_copy(
            src_ref=piece,
            dst_ref=piece,
            send_sem=hand_sem.at[KIND[name]],
            recv_sem=take_sem.at[KIND[name]],
            device_id={"zero": twin},
            device_id_type=MESH,
        ).start()

    def send(name, way, step):
        ring_copy(name, way, step).start()

    def drain(sem, *refs):
        for ref in refs:
            pltpu.make_async_copy(ref, ref, sem).wait()

    own = pl.ds(pl.multiple_of(192 * zero, 64), 192)
    for i in (0, 1, 2):
        loads[i].wait()
    k_all[own, :] = merged(wk_v[...], lk_v[...], hk_v[...])
    loads[3].wait()
    loads[4].wait()
    n_all[col, zero] = jnp.zeros((1, 128), F32)
    n_all[col, zero, :, 0:48] = nt_v[...] + ns_v[...]
    row_copy = pltpu.make_async_remote_copy(
        src_ref=n_all.at[col, zero],
        dst_ref=n_all.at[col, zero],
        send_sem=norm_sem.at[0],
        recv_sem=norm_sem.at[1],
        device_id={"zero": 0},
        device_id_type=MESH,
    )
    pl.semaphore_wait(barrier, jnp.where(is_root, 6, 4))
    send("k", 0, 0)
    send("k", 1, 0)
    for i in (5, 6, 7):
        loads[i].wait()
    v_all[own, :] = merged(wv_v[...], lv_v[...], hv_v[...])
    send("v", 0, 0)
    for i in (8, 9, 10):
        loads[i].wait()
    q_all[own, :] = merged(wq_v[...], lq_v[...], hq_v[...])
    send("q", 0, 0)
    send("q", 1, 0)

    @pl.when(jnp.logical_not(is_root))
    def _():
        row_copy.start()

    pair = [
        pltpu.make_async_remote_copy(
            src_ref=src,
            dst_ref=dst,
            send_sem=pair_sem.at[0, i],
            recv_sem=pair_sem.at[1, i],
            device_id={"zero": twin},
            device_id_type=MESH,
        )
        for i, (src, dst) in enumerate(
            ((wm.at[:, other_half], wm_v.at[my_rows]), (hm, hm_v.at[core]))
        )
    ]
    for copy in pair:
        copy.start()
    for name in ("k", "v", "q"):
        give(name, 0, -1)

    for i in (11, 12, 13):
        loads[i].wait()
    twin_rows = pl.ds(pl.multiple_of(192 * (1 - core), 64), 192)
    for i, dst in enumerate((wm_v.at[twin_rows], hm_v.at[1 - core])):
        pltpu.make_async_remote_copy(
            src_ref=dst,
            dst_ref=dst,
            send_sem=pair_sem.at[0, i],
            recv_sem=pair_sem.at[1, i],
            device_id={"zero": twin},
            device_id_type=MESH,
        ).wait_recv()
    row = lax.broadcasted_iota(jnp.int32, (192, 384), 0)
    lane = lax.broadcasted_iota(jnp.int32, (192, 384), 1)
    high = sum(
        jnp.dot(
            hm_v[c], (lane == row + 192 * c).astype(BF16), preferred_element_type=F32
        )
        for c in (0, 1)
    ).astype(BF16)
    for i in (0, 1, 2):
        lanes = slice(128 * i, 128 * i + 128)
        base = wm_v[:, lanes].astype(F32).T
        m_all[chip, pl.ds(pl.multiple_of(384 * core + 128 * i, 128), 128)] = merged(
            base, lm_v[:, lanes], high
        )
    send("m", 0, 0)
    send("m", 1, 0)
    send("v", 1, 0)
    give("m", 0, -1)
    for copy in pair:
        copy.wait_send()

    def meet_columns():
        drain(norm_sem.at[1], n_all.at[0, 0:15])
        for far in (1, 2, 3):
            pltpu.make_async_remote_copy(
                src_ref=n_all.at[col],
                dst_ref=n_all.at[col],
                send_sem=norm_sem.at[2],
                recv_sem=norm_sem.at[3],
                device_id={"cols": lax.rem(col + far, 4)},
                device_id_type=MESH,
            ).start()

    def assemble():
        drain(norm_sem.at[3], n_all.at[0:3])
        at = lax.broadcasted_iota(jnp.int32, (1, 128), 1)
        for g in range(8):
            e = [n_all[i % 4, 2 * g + i // 4] for i in range(8)]
            r = [pltpu.roll(e[i], (48 * i) % 128, 1) for i in range(8)]
            n_wide[3 * g : 3 * g + 1, :] = jnp.where(
                at < 48, r[0], jnp.where(at < 96, r[1], r[2])
            )
            n_wide[3 * g + 1 : 3 * g + 2, :] = jnp.where(
                at < 16,
                r[2],
                jnp.where(at < 64, r[3], jnp.where(at < 112, r[4], r[5])),
            )
            n_wide[3 * g + 2 : 3 * g + 3, :] = jnp.where(
                at < 32, r[5], jnp.where(at < 80, r[6], r[7])
            )
        n_out[...] = n_wide[...].astype(BF16)

    def norm_copy(to):
        return pltpu.make_async_remote_copy(
            src_ref=n_out,
            dst_ref=n_out,
            send_sem=norm_sem.at[4],
            recv_sem=norm_sem.at[5],
            device_id={"zero": to},
            device_id_type=MESH,
        )

    def spread():
        for to in (1, 2, 14, 4, 12, 6, 10, 8):
            norm_copy(to).start()

    at_root = {2: meet_columns, 4: assemble, 6: spread}

    for step in range(3):
        for n, (name, way) in enumerate(by_arrival(ORDER)):
            arrival(name, way, step).wait_recv()
            if step < 2:
                send(name, way, step + 1)
            elif name == LAST[way][-2]:
                send(name, way, 3)
                send(LAST[way][-1], way, 3)
            elif name == LAST[way][0]:
                send(name, way, 3)
            give(name, way, step)
            if step == 0 and n in at_root:
                pl.when(is_root)(at_root[n])
    last = by_arrival(LAST)
    for name, way in last[:-2]:
        arrival(name, way, 3).wait_recv()
        give(name, way, 3)

    @pl.when(is_root)
    def _():
        drain(norm_sem.at[2], n_all.at[0:3])
        drain(norm_sem.at[4], q_all.at[0:32])

    @pl.when(jnp.logical_not(is_root))
    def _():
        row_copy.wait_send()
        norm_copy(twin).wait_recv()

    @pl.when(jnp.logical_and(core == 0, jnp.logical_not(is_root)))
    def _():
        norm_copy(twin).start()
        norm_copy(twin).wait_send()

    for name, way in last[-2:]:
        arrival(name, way, 3).wait_recv()
        give(name, way, 3)
    for way in (0, 1):
        drain(send_sem.at[way], q_all.at[0:1792])
    for kind in (0, 1):
        drain(hand_sem.at[kind], q_all.at[0:2048])
        drain(take_sem.at[kind], q_all.at[0:2048])


def store_kernel(q, k, v, m, n, q_out, k_out, v_out, m_out, n_out, sem):
    parts = [
        (q.at[pl.ds(768 * i, 768)], q_out.at[pl.ds(768 * i, 768)], 0) for i in range(4)
    ]
    parts += [(m.at[i], m_out.at[:, pl.ds(384 * i, 384)], 1) for i in range(8)]
    parts += [(k, k_out, 2), (v, v_out, 3), (n, n_out, 4)]
    for src, dst, i in parts:
        pltpu.make_async_copy(src, dst, sem.at[i]).start()
    for i, (src, dst) in enumerate(
        ((q, q_out), (m_out, m_out), (k, k_out), (v, v_out), (n, n_out))
    ):
        pltpu.make_async_copy(src, dst, sem.at[i]).wait()


def on_device(wq, lq, hq, wk, lk, hk, wv, lv, hv, wm, lm, hm, nt, ns):
    anywhere = pl.BlockSpec(memory_space=pltpu.HBM)
    onchip = pl.BlockSpec(memory_space=pltpu.VMEM)
    held = pl.pallas_call(
        gather_kernel,
        out_shape=(
            pltpu.VMEM((3072, 768), BF16),
            pltpu.VMEM((3072, 256), BF16),
            pltpu.VMEM((3072, 256), BF16),
            pltpu.VMEM((8, 768, 384), BF16),
            pltpu.VMEM((24, 128), BF16),
        ),
        in_specs=[anywhere] * 14,
        out_specs=(onchip,) * 5,
        scratch_shapes=[
            pltpu.VMEM((192, 768), BF16),
            pltpu.VMEM((32, 192), BF16),
            pltpu.VMEM((32, 768), BF16),
            pltpu.VMEM((192, 256), BF16),
            pltpu.VMEM((32, 192), BF16),
            pltpu.VMEM((32, 256), BF16),
            pltpu.VMEM((192, 256), BF16),
            pltpu.VMEM((32, 192), BF16),
            pltpu.VMEM((32, 256), BF16),
            pltpu.VMEM((384, 384), BF16),
            pltpu.VMEM((32, 384), BF16),
            pltpu.VMEM((2, 32, 192), BF16),
            pltpu.VMEM((1, 48), F32),
            pltpu.VMEM((1, 48), F32),
            pltpu.VMEM((4, 16, 1, 128), F32),
            pltpu.VMEM((24, 128), F32),
            pltpu.SemaphoreType.DMA((14,)),
            pltpu.SemaphoreType.DMA((2, 2)),
            pltpu.SemaphoreType.DMA((2,)),
            pltpu.SemaphoreType.DMA((7 * len(PIECES),)),
            pltpu.SemaphoreType.DMA((2,)),
            pltpu.SemaphoreType.DMA((2,)),
            pltpu.SemaphoreType.DMA((6,)),
        ],
        compiler_params=pltpu.CompilerParams(
            collective_id=0, has_side_effects=True, vmem_limit_bytes=54400000
        ),
        name="merge_and_gather",
    )(
        wq, lq.T, hq, wk, lk.T, hk, wv, lv.T, hv, wm.T, lm.T, hm,
        nt.reshape(1, 48), ns.reshape(1, 48),
    )
    q, k, v, m, norm = pl.pallas_call(
        store_kernel,
        out_shape=(
            jax.ShapeDtypeStruct((3072, 768), BF16),
            jax.ShapeDtypeStruct((3072, 256), BF16),
            jax.ShapeDtypeStruct((3072, 256), BF16),
            jax.ShapeDtypeStruct((768, 3072), BF16),
            jax.ShapeDtypeStruct((24, 128), BF16),
        ),
        in_specs=[onchip] * 5,
        out_specs=(anywhere,) * 5,
        scratch_shapes=[pltpu.SemaphoreType.DMA((5,))],
        compiler_params=pltpu.CompilerParams(vmem_limit_bytes=24 * 2**20),
        name="store",
    )(*held)
    return q, k, v, m, norm.reshape(3072)


def solution(mesh):
    placed = (
        P(("job", "zero"), "cols"),
        P(("job", "zero"), None),
        P("job", "cols"),
        P(("job", "zero"), "cols"),
        P(("job", "zero"), None),
        P("job", "cols"),
        P(("job", "zero"), "cols"),
        P(("job", "zero"), None),
        P("job", "cols"),
        P(("job", "cols"), "zero"),
        P(("job", "cols"), None),
        P("job", "zero"),
        P(("job", "zero", "cols")),
        P(("job", "zero", "cols")),
    )
    return jax.shard_map(
        on_device,
        mesh=mesh,
        in_specs=placed,
        out_specs=(
            P("job", "cols"),
            P("job", "cols"),
            P("job", "cols"),
            P(("job", "cols"), None),
            P("job"),
        ),
        check_vma=False,
    )
```

```python
import functools

import jax
import jax.numpy as jnp
from jax import lax
from jax.experimental import pallas as pl
from jax.experimental.pallas import tpu as pltpu
from jax.sharding import PartitionSpec as P

mix_rate = 2.0
MESH = pl.DeviceIdType.MESH
BF16 = jnp.bfloat16
F32 = jnp.float32

PIECES = ("k", "v", "q", "m")
ORDER = (("k", "v", "q", "m"), ("k", "q", "m", "v"))
LAST = (("q", "v"), ("m", "k"))
UP = {"q": 4, "v": 4, "k": 3, "m": 3}
KIND = {"q": 0, "k": 0, "v": 1, "m": 1}
SIZE = {"q": 288, "k": 96, "v": 96, "m": 288}


def by_arrival(orders):
    timed = []
    for way, order in enumerate(orders):
        at = 0
        for name in order:
            at += SIZE[name]
            timed.append((at, way, name))
    return [(name, way) for _, way, name in sorted(timed)]


def merged(base, low_turned, high):
    delta = lax.dot_general(
        low_turned, high, (((0,), (0,)), ((), ())), preferred_element_type=F32
    )
    return (base.astype(F32) + mix_rate * delta).astype(BF16)


def gather_kernel(
    wq, lq, hq, wk, lk, hk, wv, lv, hv, wm, lm, hm, nt, ns,
    q_all, k_all, v_all, m_all, n_out,
    wq_v, lq_v, hq_v, wk_v, lk_v, hk_v, wv_v, lv_v, hv_v, wm_v, lm_v, hm_v, nt_v, ns_v,
    n_all, n_wide,
    load_sem, pair_sem, send_sem, recv_sem, hand_sem, take_sem, norm_sem, ready_sem,
):
    zero = lax.axis_index("zero")
    col = lax.axis_index("cols")
    core = lax.rem(zero, 2)
    chip = lax.div(zero, 2)
    above = lax.rem(zero + 2, 16)
    below = lax.rem(zero + 14, 16)
    twin = zero + 1 - 2 * core

    barrier = pltpu.get_barrier_semaphore()

    def greet(peer):
        pl.semaphore_signal(
            barrier, inc=1, device_id={"zero": peer}, device_id_type=MESH
        )

    greet(twin)
    pl.when(chip != 7)(lambda: greet(above))
    pl.when(jnp.logical_or(chip == 0, chip >= 5))(lambda: greet(below))

    is_root = zero == 0

    @pl.when(is_root)
    def _():
        for other in range(1, 16):
            greet(other)
        for far in (1, 2, 3):
            pl.semaphore_signal(
                barrier,
                inc=1,
                device_id={"cols": lax.rem(col + far, 4)},
                device_id_type=MESH,
            )

    half = pl.ds(pl.multiple_of(384 * core, 128), 384)
    other_half = pl.ds(pl.multiple_of(384 * (1 - core), 128), 384)
    my_rows = pl.ds(pl.multiple_of(192 * core, 64), 192)
    loads = [
        pltpu.make_async_copy(src, dst, load_sem.at[i])
        for i, (src, dst) in enumerate(
            (
                (lk, lk_v),
                (hk, hk_v),
                (wk, wk_v),
                (nt, nt_v),
                (ns, ns_v),
                (lv, lv_v),
                (hv, hv_v),
                (wv, wv_v),
                (lq, lq_v),
                (hq, hq_v),
                (wq, wq_v),
                (hm, hm_v.at[core]),
                (wm.at[:, half], wm_v.at[my_rows]),
                (lm.at[:, half], lm_v),
            )
        )
    ]
    for load in loads:
        load.start()

    def place(name, origin, of):
        if name == "m":
            return m_all.at[origin, pl.ds(pl.multiple_of(384 * of, 128), 384)]
        rows = pl.ds(pl.multiple_of(192 * (2 * origin + of), 64), 192)
        return {"q": q_all, "k": k_all, "v": v_all}[name].at[rows]

    arrivals = [
        (name, way, step)
        for way in (0, 1)
        for name in PIECES
        for step in range(UP[name] if way == 0 else 7 - UP[name])
    ] + [("v", 1, 3)]

    def arrived_from(way, step):
        return lax.rem(chip + (7 - step if way == 0 else step + 1), 8)

    def ring_copy(name, way, step):
        origin = lax.rem(chip + (8 - step if way == 0 else step), 8)
        piece = place(name, origin, core)
        return pltpu.make_async_remote_copy(
            src_ref=piece,
            dst_ref=piece,
            send_sem=send_sem.at[way],
            recv_sem=recv_sem.at[arrivals.index((name, way, step))],
            device_id={"zero": above if way == 0 else below},
            device_id_type=MESH,
        )

    def arrival(name, way, step):
        piece = place(name, arrived_from(way, step), core)
        return pltpu.make_async_remote_copy(
            src_ref=piece,
            dst_ref=piece,
            send_sem=send_sem.at[way],
            recv_sem=recv_sem.at[arrivals.index((name, way, step))],
            device_id={"zero": below if way == 0 else above},
            device_id_type=MESH,
        )

    def give(name, way, step):
        origin = chip if step < 0 else arrived_from(way, step)
        piece = place(name, origin, core)
        pltpu.make_async_remote_copy(
            src_ref=piece,
            dst_ref=piece,
            send_sem=hand_sem.at[KIND[name]],
            recv_sem=take_sem.at[KIND[name]],
            device_id={"zero": twin},
            device_id_type=MESH,
        ).start()

    def send(name, way, step):
        ring_copy(name, way, step).start()

    def drain(sem, *refs):
        for ref in refs:
            pltpu.make_async_copy(ref, ref, sem).wait()

    own = pl.ds(pl.multiple_of(192 * zero, 64), 192)
    for i in (0, 1, 2):
        loads[i].wait()
    k_all[own, :] = merged(wk_v[...], lk_v[...], hk_v[...])
    loads[3].wait()
    loads[4].wait()
    n_all[col, zero] = jnp.zeros((1, 128), F32)
    n_all[col, zero, :, 0:48] = nt_v[...] + ns_v[...]
    row_copy = pltpu.make_async_remote_copy(
        src_ref=n_all.at[col, zero],
        dst_ref=n_all.at[col, zero],
        send_sem=norm_sem.at[0],
        recv_sem=norm_sem.at[1],
        device_id={"zero": 0},
        device_id_type=MESH,
    )
    pair = [
        pltpu.make_async_remote_copy(
            src_ref=src,
            dst_ref=dst,
            send_sem=pair_sem.at[0, i],
            recv_sem=pair_sem.at[1, i],
            device_id={"zero": twin},
            device_id_type=MESH,
        )
        for i, (src, dst) in enumerate(
            ((wm.at[:, other_half], wm_v.at[my_rows]), (hm, hm_v.at[core]))
        )
    ]
    pl.semaphore_wait(
        barrier,
        1
        + jnp.where(chip == 0, 0, 1)
        + jnp.where(chip >= 4, 1, 0)
        + jnp.where(is_root, 3, 1),
    )

    def ready(peer, i):
        pl.semaphore_signal(
            ready_sem.at[i], inc=1, device_id={"zero": peer}, device_id_type=MESH
        )

    pl.when(jnp.logical_and(chip >= 1, chip <= 4))(lambda: ready(below, 0))
    pl.when(chip == 7)(lambda: ready(above, 1))
    first = chip == 0
    early = jnp.logical_and(chip >= 1, chip <= 3)
    late = chip >= 4

    @pl.when(first)
    def _():
        pl.semaphore_wait(ready_sem.at[0], 1)
        send("k", 0, 0)

    @pl.when(jnp.logical_not(first))
    def _():
        send("k", 1, 0)

    pl.when(late)(lambda: send("k", 0, 0))
    for copy in pair:
        copy.start()
    for i in (5, 6, 7):
        loads[i].wait()
    v_all[own, :] = merged(wv_v[...], lv_v[...], hv_v[...])
    for i in (8, 9, 10):
        loads[i].wait()
    q_all[own, :] = merged(wq_v[...], lq_v[...], hq_v[...])

    @pl.when(jnp.logical_not(first))
    def _():
        send("q", 1, 0)

    @pl.when(early)
    def _():
        pl.semaphore_wait(ready_sem.at[0], 1)
        send("k", 0, 0)

    send("v", 0, 0)
    send("q", 0, 0)

    @pl.when(first)
    def _():
        pl.semaphore_wait(ready_sem.at[1], 1)
        send("k", 1, 0)
        send("q", 1, 0)

    @pl.when(jnp.logical_not(is_root))
    def _():
        row_copy.start()

    for name in ("k", "v", "q"):
        give(name, 0, -1)

    for i in (11, 12, 13):
        loads[i].wait()
    twin_rows = pl.ds(pl.multiple_of(192 * (1 - core), 64), 192)
    for i, dst in enumerate((wm_v.at[twin_rows], hm_v.at[1 - core])):
        pltpu.make_async_remote_copy(
            src_ref=dst,
            dst_ref=dst,
            send_sem=pair_sem.at[0, i],
            recv_sem=pair_sem.at[1, i],
            device_id={"zero": twin},
            device_id_type=MESH,
        ).wait_recv()
    row = lax.broadcasted_iota(jnp.int32, (192, 384), 0)
    lane = lax.broadcasted_iota(jnp.int32, (192, 384), 1)
    high = sum(
        jnp.dot(
            hm_v[c], (lane == row + 192 * c).astype(BF16), preferred_element_type=F32
        )
        for c in (0, 1)
    ).astype(BF16)
    for i in (0, 1, 2):
        lanes = slice(128 * i, 128 * i + 128)
        base = wm_v[:, lanes].astype(F32).T
        m_all[chip, pl.ds(pl.multiple_of(384 * core + 128 * i, 128), 128)] = merged(
            base, lm_v[:, lanes], high
        )
    send("m", 0, 0)
    send("m", 1, 0)
    send("v", 1, 0)
    give("m", 0, -1)
    for copy in pair:
        copy.wait_send()

    def meet_columns():
        drain(norm_sem.at[1], n_all.at[0, 0:15])
        for far in (1, 2, 3):
            pltpu.make_async_remote_copy(
                src_ref=n_all.at[col],
                dst_ref=n_all.at[col],
                send_sem=norm_sem.at[2],
                recv_sem=norm_sem.at[3],
                device_id={"cols": lax.rem(col + far, 4)},
                device_id_type=MESH,
            ).start()

    def assemble():
        drain(norm_sem.at[3], n_all.at[0:3])
        at = lax.broadcasted_iota(jnp.int32, (1, 128), 1)
        for g in range(8):
            e = [n_all[i % 4, 2 * g + i // 4] for i in range(8)]
            r = [pltpu.roll(e[i], (48 * i) % 128, 1) for i in range(8)]
            n_wide[3 * g : 3 * g + 1, :] = jnp.where(
                at < 48, r[0], jnp.where(at < 96, r[1], r[2])
            )
            n_wide[3 * g + 1 : 3 * g + 2, :] = jnp.where(
                at < 16,
                r[2],
                jnp.where(at < 64, r[3], jnp.where(at < 112, r[4], r[5])),
            )
            n_wide[3 * g + 2 : 3 * g + 3, :] = jnp.where(
                at < 32, r[5], jnp.where(at < 80, r[6], r[7])
            )
        n_out[...] = n_wide[...].astype(BF16)

    def norm_copy(to):
        return pltpu.make_async_remote_copy(
            src_ref=n_out,
            dst_ref=n_out,
            send_sem=norm_sem.at[4],
            recv_sem=norm_sem.at[5],
            device_id={"zero": to},
            device_id_type=MESH,
        )

    def spread():
        for to in (1, 2, 14, 4, 12, 6, 10, 8):
            norm_copy(to).start()

    at_root = {2: meet_columns, 4: assemble, 6: spread}

    for step in range(3):
        for n, (name, way) in enumerate(by_arrival(ORDER)):
            arrival(name, way, step).wait_recv()
            if step < 2:
                send(name, way, step + 1)
            elif (name, way) == ("q", 0):
                send("q", 0, 3)
                pl.when(chip != 7)(lambda: send("v", 0, 3))
            elif (name, way) == ("m", 1):
                send("m", 1, 3)
                send("k", 1, 3)
            elif (name, way) == ("v", 1):
                pl.when(chip == 1)(lambda: send("v", 1, 3))
            give(name, way, step)
            if step == 0 and n in at_root:
                pl.when(is_root)(at_root[n])
    last = by_arrival(LAST)
    for name, way in last[:-2]:
        arrival(name, way, 3).wait_recv()
        give(name, way, 3)

    @pl.when(is_root)
    def _():
        drain(norm_sem.at[2], n_all.at[0:3])
        drain(norm_sem.at[4], q_all.at[0:32])

    @pl.when(jnp.logical_not(is_root))
    def _():
        row_copy.wait_send()
        norm_copy(twin).wait_recv()

    @pl.when(jnp.logical_and(core == 0, jnp.logical_not(is_root)))
    def _():
        norm_copy(twin).start()
        norm_copy(twin).wait_send()

    arrival("k", 1, 3).wait_recv()
    give("k", 1, 3)

    def end_up():
        arrival("v", 0, 3).wait_recv()
        give("v", 0, 3)

    def end_down():
        arrival("v", 1, 3).wait_recv()
        give("v", 1, 3)

    pl.when(jnp.logical_not(first))(end_up)
    pl.when(first)(end_down)
    pl.when(chip != 7)(lambda: drain(send_sem.at[0], q_all.at[0:1792]))
    pl.when(chip == 7)(lambda: drain(send_sem.at[0], q_all.at[0:1728]))
    pl.when(chip != 1)(lambda: drain(send_sem.at[1], q_all.at[0:1792]))
    pl.when(chip == 1)(lambda: drain(send_sem.at[1], q_all.at[0:1856]))
    for kind in (0, 1):
        drain(hand_sem.at[kind], q_all.at[0:2048])
        drain(take_sem.at[kind], q_all.at[0:2048])


def store_kernel(q, k, v, m, n, q_out, k_out, v_out, m_out, n_out, sem):
    parts = [
        (q.at[pl.ds(768 * i, 768)], q_out.at[pl.ds(768 * i, 768)], 0) for i in range(4)
    ]
    parts += [(m.at[i], m_out.at[:, pl.ds(384 * i, 384)], 1) for i in range(8)]
    parts += [(k, k_out, 2), (v, v_out, 3), (n, n_out, 4)]
    for src, dst, i in parts:
        pltpu.make_async_copy(src, dst, sem.at[i]).start()
    for i, (src, dst) in enumerate(
        ((q, q_out), (m_out, m_out), (k, k_out), (v, v_out), (n, n_out))
    ):
        pltpu.make_async_copy(src, dst, sem.at[i]).wait()


def on_device(wq, lq, hq, wk, lk, hk, wv, lv, hv, wm, lm, hm, nt, ns):
    anywhere = pl.BlockSpec(memory_space=pltpu.HBM)
    onchip = pl.BlockSpec(memory_space=pltpu.VMEM)
    held = pl.pallas_call(
        gather_kernel,
        out_shape=(
            pltpu.VMEM((3072, 768), BF16),
            pltpu.VMEM((3072, 256), BF16),
            pltpu.VMEM((3072, 256), BF16),
            pltpu.VMEM((8, 768, 384), BF16),
            pltpu.VMEM((24, 128), BF16),
        ),
        in_specs=[anywhere] * 14,
        out_specs=(onchip,) * 5,
        scratch_shapes=[
            pltpu.VMEM((192, 768), BF16),
            pltpu.VMEM((32, 192), BF16),
            pltpu.VMEM((32, 768), BF16),
            pltpu.VMEM((192, 256), BF16),
            pltpu.VMEM((32, 192), BF16),
            pltpu.VMEM((32, 256), BF16),
            pltpu.VMEM((192, 256), BF16),
            pltpu.VMEM((32, 192), BF16),
            pltpu.VMEM((32, 256), BF16),
            pltpu.VMEM((384, 384), BF16),
            pltpu.VMEM((32, 384), BF16),
            pltpu.VMEM((2, 32, 192), BF16),
            pltpu.VMEM((1, 48), F32),
            pltpu.VMEM((1, 48), F32),
            pltpu.VMEM((4, 16, 1, 128), F32),
            pltpu.VMEM((24, 128), F32),
            pltpu.SemaphoreType.DMA((14,)),
            pltpu.SemaphoreType.DMA((2, 2)),
            pltpu.SemaphoreType.DMA((2,)),
            pltpu.SemaphoreType.DMA((7 * len(PIECES) + 1,)),
            pltpu.SemaphoreType.DMA((2,)),
            pltpu.SemaphoreType.DMA((2,)),
            pltpu.SemaphoreType.DMA((6,)),
            pltpu.SemaphoreType.REGULAR((2,)),
        ],
        compiler_params=pltpu.CompilerParams(
            collective_id=0, has_side_effects=True, vmem_limit_bytes=54400000
        ),
        name="merge_and_gather",
    )(
        wq, lq.T, hq, wk, lk.T, hk, wv, lv.T, hv, wm.T, lm.T, hm,
        nt.reshape(1, 48), ns.reshape(1, 48),
    )
    q, k, v, m, norm = pl.pallas_call(
        store_kernel,
        out_shape=(
            jax.ShapeDtypeStruct((3072, 768), BF16),
            jax.ShapeDtypeStruct((3072, 256), BF16),
            jax.ShapeDtypeStruct((3072, 256), BF16),
            jax.ShapeDtypeStruct((768, 3072), BF16),
            jax.ShapeDtypeStruct((24, 128), BF16),
        ),
        in_specs=[onchip] * 5,
        out_specs=(anywhere,) * 5,
        scratch_shapes=[pltpu.SemaphoreType.DMA((5,))],
        compiler_params=pltpu.CompilerParams(vmem_limit_bytes=24 * 2**20),
        name="store",
    )(*held)
    return q, k, v, m, norm.reshape(3072)


def solution(mesh):
    placed = (
        P(("job", "zero"), "cols"),
        P(("job", "zero"), None),
        P("job", "cols"),
        P(("job", "zero"), "cols"),
        P(("job", "zero"), None),
        P("job", "cols"),
        P(("job", "zero"), "cols"),
        P(("job", "zero"), None),
        P("job", "cols"),
        P(("job", "cols"), "zero"),
        P(("job", "cols"), None),
        P("job", "zero"),
        P(("job", "zero", "cols")),
        P(("job", "zero", "cols")),
    )
    return jax.shard_map(
        on_device,
        mesh=mesh,
        in_specs=placed,
        out_specs=(
            P("job", "cols"),
            P("job", "cols"),
            P("job", "cols"),
            P(("job", "cols"), None),
            P("job"),
        ),
        check_vma=False,
    )
```

```python
import functools

import jax
import jax.numpy as jnp
from jax import lax
from jax.experimental import pallas as pl
from jax.experimental.pallas import tpu as pltpu
from jax.sharding import PartitionSpec as P

mix_rate = 2.0
MESH = pl.DeviceIdType.MESH
BF16 = jnp.bfloat16
F32 = jnp.float32

ROOT = 1
MIDDLE, MIDDLE_OF_4 = 192, 64


def merged(base, low_turned, high):
    delta = lax.dot_general(
        low_turned, high, (((0,), (0,)), ((), ())), preferred_element_type=F32
    )
    return (base.astype(F32) + mix_rate * delta).astype(BF16)


def gather_kernel(*refs):
    pl.run_scoped(
        functools.partial(gather, *refs),
        load_sem=pltpu.SemaphoreType.DMA((14,)),
        pair_sent=pltpu.SemaphoreType.DMA((2,)),
        send_sem=pltpu.SemaphoreType.DMA((2, 2)),
        hand_sem=pltpu.SemaphoreType.DMA((2,)),
        norm_sent=pltpu.SemaphoreType.DMA((3,)),
        pair_sem=pltpu.SemaphoreType.DMA((2,)),
        recv_sem=pltpu.SemaphoreType.DMA((2, 9)),
        take_sem=pltpu.SemaphoreType.DMA((2,)),
        norm_sem=pltpu.SemaphoreType.DMA((3,)),
        ready_sem=pltpu.SemaphoreType.REGULAR((2,)),
    )


def gather(
    wq, lq, hq, wk, lk, hk, wv, lv, hv, wm, lm, hm, nt, ns,
    w_all, m_all, n_out,
    wq_v, lq_v, hq_v, wk_v, lk_v, hk_v, wv_v, lv_v, hv_v, wm_v, lm_v, hm_v, nt_v, ns_v,
    n_all, n_wide,
    load_sem, pair_sent, send_sem, hand_sem, norm_sent,
    pair_sem, recv_sem, take_sem, norm_sem, ready_sem,
):
    zero = lax.axis_index("zero")
    col = lax.axis_index("cols")
    core = lax.rem(zero, 2)
    chip = lax.div(zero, 2)
    above = lax.rem(zero + 2, 16)
    below = lax.rem(zero + 14, 16)
    twin = zero + 1 - 2 * core

    half = pl.ds(pl.multiple_of(384 * core, 128), 384)
    other_half = pl.ds(pl.multiple_of(384 * (1 - core), 128), 384)
    my_rows = pl.ds(pl.multiple_of(192 * core, 64), 192)
    loads = [
        pltpu.make_async_copy(src, dst, load_sem.at[i])
        for i, (src, dst) in enumerate(
            (
                (lk, lk_v),
                (hk, hk_v),
                (wk, wk_v),
                (nt, nt_v),
                (ns, ns_v),
                (lv, lv_v),
                (hv, hv_v),
                (wv, wv_v),
                (lq, lq_v),
                (hq, hq_v),
                (wq, wq_v),
                (hm, hm_v.at[core]),
                (wm.at[:, half], wm_v.at[my_rows]),
                (lm.at[:, half], lm_v),
            )
        )
    ]
    for load in loads[:3]:
        load.start()

    barrier = pltpu.get_barrier_semaphore()

    def greet(peer):
        pl.semaphore_signal(
            barrier, inc=1, device_id={"zero": peer}, device_id_type=MESH
        )

    greet(twin)
    pl.when(chip != 7)(lambda: greet(above))
    pl.when(jnp.logical_or(chip == 0, chip >= 5))(lambda: greet(below))

    is_root = zero == ROOT

    @pl.when(is_root)
    def _():
        for other in range(16):
            if other != ROOT:
                greet(other)
        for far in (1, 2, 3):
            pl.semaphore_signal(
                barrier,
                inc=1,
                device_id={"cols": lax.rem(col + far, 4)},
                device_id_type=MESH,
            )

    for load in loads[3:]:
        load.start()

    def rows_of(origin, of, start=0, size=192):
        return pl.ds(pl.multiple_of(192 * (2 * origin + of) + start, 32), size)

    def slab(origin, of, start=0, size=384):
        return m_all.at[
            origin, pl.ds(pl.multiple_of(384 * of + start, 64), size)
        ]

    def piece(name, origin, way=0):
        if name == "k":
            return w_all.at[rows_of(origin, core), pl.ds(0, 256)]
        if name == "vq":
            return w_all.at[rows_of(origin, core), pl.ds(256, 1024)]
        if name == "w":
            return w_all.at[rows_of(origin, core)]
        if name == "m":
            return slab(origin, core)
        if name == "w half":
            return w_all.at[rows_of(origin, core, 96 * way, 96)]
        middle = MIDDLE_OF_4 if name == "m part of 4" else MIDDLE
        return slab(
            origin, core, middle * way, 384 - middle if way else middle
        )

    slots = {
        0: {"k": 0, "vq": 1, "m": 2},
        1: {"w": 3, "m": 4},
        2: {"w": 5, "m": 6},
        3: {"w half": 7, "m half": 8, "m part of 4": 8},
    }

    def arrived_from(way, step):
        return lax.rem(chip + (7 - step if way == 0 else step + 1), 8)

    def copy_of(name, way, step, origin, to):
        ref = piece(name, origin, way)
        return pltpu.make_async_remote_copy(
            src_ref=ref,
            dst_ref=ref,
            send_sem=send_sem.at[way, 1 if name[0] == "m" else 0],
            recv_sem=recv_sem.at[way, slots[step][name]],
            device_id={"zero": to},
            device_id_type=MESH,
        )

    def send(name, way, step):
        origin = chip if step == 0 else arrived_from(way, step - 1)
        copy_of(name, way, step, origin, above if way == 0 else below).start()

    def arrive(name, way, step):
        origin = arrived_from(way, step)
        copy_of(name, way, step, origin, twin).wait_recv()
        hand(name, origin, way)

    def hand(name, origin, way=0):
        ref = piece(name, origin, way)
        kind = 1 if name[0] == "m" else 0
        pltpu.make_async_remote_copy(
            src_ref=ref,
            dst_ref=ref,
            send_sem=hand_sem.at[kind],
            recv_sem=take_sem.at[kind],
            device_id={"zero": twin},
            device_id_type=MESH,
        ).start()

    def drain(sem, *refs):
        for ref in refs:
            pltpu.make_async_copy(ref, ref, sem).wait()

    own = rows_of(chip, core)
    for i in (0, 1, 2):
        loads[i].wait()
    w_all[own, 0:256] = merged(wk_v[...], lk_v[...], hk_v[...])
    loads[3].wait()
    loads[4].wait()
    n_all[col, zero] = jnp.zeros((1, 128), F32)
    n_all[col, zero, :, 0:48] = nt_v[...] + ns_v[...]
    row_copy = pltpu.make_async_remote_copy(
        src_ref=n_all.at[col, zero],
        dst_ref=n_all.at[col, zero],
        send_sem=norm_sent.at[0],
        recv_sem=norm_sem.at[0],
        device_id={"zero": ROOT},
        device_id_type=MESH,
    )
    pair = [
        pltpu.make_async_remote_copy(
            src_ref=src,
            dst_ref=dst,
            send_sem=pair_sent.at[i],
            recv_sem=pair_sem.at[i],
            device_id={"zero": twin},
            device_id_type=MESH,
        )
        for i, (src, dst) in enumerate(
            ((wm.at[:, other_half], wm_v.at[my_rows]), (hm, hm_v.at[core]))
        )
    ]
    pl.semaphore_wait(
        barrier,
        1
        + jnp.where(chip == 0, 0, 1)
        + jnp.where(chip >= 4, 1, 0)
        + jnp.where(is_root, 3, 1),
    )

    def ready(peer, i):
        pl.semaphore_signal(
            ready_sem.at[i], inc=1, device_id={"zero": peer}, device_id_type=MESH
        )

    pl.when(jnp.logical_and(chip >= 1, chip <= 4))(lambda: ready(below, 0))
    pl.when(chip == 7)(lambda: ready(above, 1))
    first = chip == 0
    early = jnp.logical_and(chip >= 1, chip <= 3)
    late = chip >= 4

    @pl.when(first)
    def _():
        pl.semaphore_wait(ready_sem.at[0], 1)
        send("k", 0, 0)

    @pl.when(jnp.logical_not(first))
    def _():
        send("k", 1, 0)

    pl.when(late)(lambda: send("k", 0, 0))
    for copy in pair:
        copy.start()
    for i in (5, 6, 7):
        loads[i].wait()
    w_all[own, 256:512] = merged(wv_v[...], lv_v[...], hv_v[...])
    for i in (8, 9, 10):
        loads[i].wait()
    w_all[own, 512:1280] = merged(wq_v[...], lq_v[...], hq_v[...])

    @pl.when(jnp.logical_not(first))
    def _():
        send("vq", 1, 0)

    @pl.when(early)
    def _():
        pl.semaphore_wait(ready_sem.at[0], 1)
        send("k", 0, 0)

    send("vq", 0, 0)

    @pl.when(first)
    def _():
        pl.semaphore_wait(ready_sem.at[1], 1)
        send("k", 1, 0)
        send("vq", 1, 0)

    @pl.when(jnp.logical_not(is_root))
    def _():
        row_copy.start()

    hand("w", chip)

    for i in (11, 12, 13):
        loads[i].wait()
    twin_rows = pl.ds(pl.multiple_of(192 * (1 - core), 64), 192)
    for i, dst in enumerate((wm_v.at[twin_rows], hm_v.at[1 - core])):
        pltpu.make_async_remote_copy(
            src_ref=dst,
            dst_ref=dst,
            send_sem=pair_sent.at[i],
            recv_sem=pair_sem.at[i],
            device_id={"zero": twin},
            device_id_type=MESH,
        ).wait_recv()
    row = lax.broadcasted_iota(jnp.int32, (192, 384), 0)
    lane = lax.broadcasted_iota(jnp.int32, (192, 384), 1)
    high = sum(
        jnp.dot(
            hm_v[c], (lane == row + 192 * c).astype(BF16), preferred_element_type=F32
        )
        for c in (0, 1)
    ).astype(BF16)
    for i in (0, 1, 2):
        lanes = slice(128 * i, 128 * i + 128)
        base = wm_v[:, lanes].astype(F32).T
        m_all[chip, pl.ds(pl.multiple_of(384 * core + 128 * i, 128), 128)] = merged(
            base, lm_v[:, lanes], high
        )
    send("m", 0, 0)
    send("m", 1, 0)
    hand("m", chip)
    for copy in pair:
        copy.wait_send()

    def meet_columns():
        drain(norm_sem.at[0], n_all.at[0, 0:15])
        for far in (1, 2, 3):
            pltpu.make_async_remote_copy(
                src_ref=n_all.at[col],
                dst_ref=n_all.at[col],
                send_sem=norm_sent.at[1],
                recv_sem=norm_sem.at[1],
                device_id={"cols": lax.rem(col + far, 4)},
                device_id_type=MESH,
            ).start()

    def assemble():
        drain(norm_sem.at[1], n_all.at[0:3])
        at = lax.broadcasted_iota(jnp.int32, (1, 128), 1)
        for g in range(8):
            e = [n_all[i % 4, 2 * g + i // 4] for i in range(8)]
            r = [pltpu.roll(e[i], (48 * i) % 128, 1) for i in range(8)]
            n_wide[3 * g : 3 * g + 1, :] = jnp.where(
                at < 48, r[0], jnp.where(at < 96, r[1], r[2])
            )
            n_wide[3 * g + 1 : 3 * g + 2, :] = jnp.where(
                at < 16,
                r[2],
                jnp.where(at < 64, r[3], jnp.where(at < 112, r[4], r[5])),
            )
            n_wide[3 * g + 2 : 3 * g + 3, :] = jnp.where(
                at < 32, r[5], jnp.where(at < 80, r[6], r[7])
            )
        n_out[...] = n_wide[...].astype(BF16)

    def norm_copy(to):
        return pltpu.make_async_remote_copy(
            src_ref=n_out,
            dst_ref=n_out,
            send_sem=norm_sent.at[2],
            recv_sem=norm_sem.at[2],
            device_id={"zero": to},
            device_id_type=MESH,
        )

    def spread():
        for to in (0, 2, 14, 4, 12, 6, 10, 8):
            norm_copy(to).start()

    ways = (0, 1)
    for way in ways:
        arrive("k", way, 0)
    pl.when(is_root)(meet_columns)
    for way in ways:
        arrive("vq", way, 0)
        send("w", way, 1)
    pl.when(is_root)(assemble)
    for way in ways:
        arrive("m", way, 0)
        send("m", way, 1)
    pl.when(is_root)(spread)
    for way in ways:
        arrive("w", way, 1)
        send("w", way, 2)
    for way in ways:
        arrive("m", way, 1)
        send("m", way, 2)
    for way in ways:
        arrive("w", way, 2)
        send("w half", way, 3)
    for way, odd_one in zip(ways, (7, 1)):
        arrive("m", way, 2)
        pl.when(chip != odd_one)(lambda: send("m half", way, 3))
        pl.when(chip == odd_one)(lambda: send("m part of 4", way, 3))
    for way in ways:
        arrive("w half", way, 3)

    @pl.when(is_root)
    def _():
        drain(norm_sent.at[1], n_all.at[0:3])
        drain(norm_sent.at[2], m_all.at[0, 0:64])

    @pl.when(jnp.logical_not(is_root))
    def _():
        row_copy.wait_send()
        norm_copy(twin).wait_recv()

    @pl.when(jnp.logical_and(core == 0, jnp.logical_not(first)))
    def _():
        norm_copy(twin).start()
        norm_copy(twin).wait_send()

    def finish(name):
        for way in ways:
            arrive(name, way, 3)

    pl.when(jnp.logical_not(first))(lambda: finish("m half"))
    pl.when(first)(lambda: finish("m part of 4"))
    for way, odd_one, rows in ((0, 7, 152), (1, 1, 184)):
        drain(send_sem.at[way, 0], w_all.at[0:672])
        pl.when(chip != odd_one)(
            lambda: drain(send_sem.at[way, 1], m_all.at[0:7, 0:192])
        )
        pl.when(chip == odd_one)(
            lambda: drain(send_sem.at[way, 1], m_all.at[:, 0:rows])
        )
    for sem in (hand_sem, take_sem):
        drain(sem.at[0], w_all.at[0:1536])
        drain(sem.at[1], m_all.at[:, 0:384])


def store_kernel(w, m, n, q_out, k_out, v_out, m_out, n_out, sem):
    parts = [(m.at[i], m_out.at[:, pl.ds(384 * i, 384)], 1) for i in range(8)]
    for i in range(4):
        rows = pl.ds(768 * i, 768)
        parts += [
            (w.at[rows, pl.ds(512, 768)], q_out.at[rows], 0),
            (w.at[rows, pl.ds(0, 256)], k_out.at[rows], 2),
            (w.at[rows, pl.ds(256, 256)], v_out.at[rows], 3),
        ]
    parts += [(n, n_out, 4)]
    for src, dst, i in parts:
        pltpu.make_async_copy(src, dst, sem.at[i]).start()
    for i, dst in enumerate((q_out, m_out, k_out, v_out, n_out)):
        pltpu.make_async_copy(dst, dst, sem.at[i]).wait()


def on_device(wq, lq, hq, wk, lk, hk, wv, lv, hv, wm, lm, hm, nt, ns):
    anywhere = pl.BlockSpec(memory_space=pltpu.HBM)
    onchip = pl.BlockSpec(memory_space=pltpu.VMEM)
    held = pl.pallas_call(
        gather_kernel,
        out_shape=(
            pltpu.VMEM((3072, 1280), BF16),
            pltpu.VMEM((8, 768, 384), BF16),
            pltpu.VMEM((24, 128), BF16),
        ),
        in_specs=[anywhere] * 14,
        out_specs=(onchip,) * 3,
        scratch_shapes=[
            pltpu.VMEM((192, 768), BF16),
            pltpu.VMEM((32, 192), BF16),
            pltpu.VMEM((32, 768), BF16),
            pltpu.VMEM((192, 256), BF16),
            pltpu.VMEM((32, 192), BF16),
            pltpu.VMEM((32, 256), BF16),
            pltpu.VMEM((192, 256), BF16),
            pltpu.VMEM((32, 192), BF16),
            pltpu.VMEM((32, 256), BF16),
            pltpu.VMEM((384, 384), BF16),
            pltpu.VMEM((32, 384), BF16),
            pltpu.VMEM((2, 32, 192), BF16),
            pltpu.VMEM((1, 48), F32),
            pltpu.VMEM((1, 48), F32),
            pltpu.VMEM((4, 16, 1, 128), F32),
            pltpu.VMEM((24, 128), F32),
        ],
        compiler_params=pltpu.CompilerParams(
            collective_id=0, has_side_effects=True, vmem_limit_bytes=54400000
        ),
        name="merge_and_gather",
    )(
        wq, lq.T, hq, wk, lk.T, hk, wv, lv.T, hv, wm.T, lm.T, hm,
        nt.reshape(1, 48), ns.reshape(1, 48),
    )
    q, k, v, m, norm = pl.pallas_call(
        store_kernel,
        out_shape=(
            jax.ShapeDtypeStruct((3072, 768), BF16),
            jax.ShapeDtypeStruct((3072, 256), BF16),
            jax.ShapeDtypeStruct((3072, 256), BF16),
            jax.ShapeDtypeStruct((768, 3072), BF16),
            jax.ShapeDtypeStruct((24, 128), BF16),
        ),
        in_specs=[onchip] * 3,
        out_specs=(anywhere,) * 5,
        scratch_shapes=[pltpu.SemaphoreType.DMA((5,))],
        compiler_params=pltpu.CompilerParams(vmem_limit_bytes=24 * 2**20),
        name="store",
    )(*held)
    return q, k, v, m, norm.reshape(3072)


def solution(mesh):
    placed = (
        P(("job", "zero"), "cols"),
        P(("job", "zero"), None),
        P("job", "cols"),
        P(("job", "zero"), "cols"),
        P(("job", "zero"), None),
        P("job", "cols"),
        P(("job", "zero"), "cols"),
        P(("job", "zero"), None),
        P("job", "cols"),
        P(("job", "cols"), "zero"),
        P(("job", "cols"), None),
        P("job", "zero"),
        P(("job", "zero", "cols")),
        P(("job", "zero", "cols")),
    )
    return jax.shard_map(
        on_device,
        mesh=mesh,
        in_specs=placed,
        out_specs=(
            P("job", "cols"),
            P("job", "cols"),
            P("job", "cols"),
            P(("job", "cols"), None),
            P("job"),
        ),
        check_vma=False,
    )
```

```python
import functools

import jax
import jax.numpy as jnp
from jax import lax
from jax.experimental import pallas as pl
from jax.experimental.pallas import tpu as pltpu
from jax.sharding import PartitionSpec as P

mix_rate = 2.0
MESH = pl.DeviceIdType.MESH
BF16 = jnp.bfloat16
F32 = jnp.float32

ROOT = 1
MIDDLE, MIDDLE_OF_4 = 192, 64


def merged(base, low_turned, high):
    delta = lax.dot_general(
        low_turned, high, (((0,), (0,)), ((), ())), preferred_element_type=F32
    )
    return (base.astype(F32) + mix_rate * delta).astype(BF16)


def gather_kernel(*refs):
    pl.run_scoped(
        functools.partial(gather, *refs),
        load_sem=pltpu.SemaphoreType.DMA((14,)),
        pair_sent=pltpu.SemaphoreType.DMA((2,)),
        send_sem=pltpu.SemaphoreType.DMA((2, 2)),
        hand_sem=pltpu.SemaphoreType.DMA((2,)),
        norm_sent=pltpu.SemaphoreType.DMA((3,)),
        pair_sem=pltpu.SemaphoreType.DMA((2,)),
        recv_sem=pltpu.SemaphoreType.DMA((2, 9)),
        take_sem=pltpu.SemaphoreType.DMA((2,)),
        norm_sem=pltpu.SemaphoreType.DMA((3,)),
        ready_sem=pltpu.SemaphoreType.REGULAR((2,)),
    )


def gather(
    wq, lq, hq, wk, lk, hk, wv, lv, hv, wm, lm, hm, nt, ns,
    w_all, m_all, n_out,
    wq_v, lq_v, hq_v, wk_v, lk_v, hk_v, wv_v, lv_v, hv_v, wm_v, lm_v, hm_v, nt_v, ns_v,
    n_all, n_wide,
    load_sem, pair_sent, send_sem, hand_sem, norm_sent,
    pair_sem, recv_sem, take_sem, norm_sem, ready_sem,
):
    zero = lax.axis_index("zero")
    col = lax.axis_index("cols")
    core = lax.rem(zero, 2)
    chip = lax.div(zero, 2)
    above = lax.rem(zero + 2, 16)
    below = lax.rem(zero + 14, 16)
    twin = zero + 1 - 2 * core

    half = pl.ds(pl.multiple_of(384 * core, 128), 384)
    other_half = pl.ds(pl.multiple_of(384 * (1 - core), 128), 384)
    my_rows = pl.ds(pl.multiple_of(192 * core, 64), 192)
    loads = [
        pltpu.make_async_copy(src, dst, load_sem.at[i])
        for i, (src, dst) in enumerate(
            (
                (lk, lk_v),
                (hk, hk_v),
                (wk, wk_v),
                (nt, nt_v),
                (ns, ns_v),
                (lv, lv_v),
                (hv, hv_v),
                (wv, wv_v),
                (lq, lq_v),
                (hq, hq_v),
                (wq, wq_v),
                (hm, hm_v.at[core]),
                (wm.at[:, half], wm_v.at[my_rows]),
                (lm.at[:, half], lm_v),
            )
        )
    ]
    for load in loads[:3]:
        load.start()

    barrier = pltpu.get_barrier_semaphore()

    def greet(peer):
        pl.semaphore_signal(
            barrier, inc=1, device_id={"zero": peer}, device_id_type=MESH
        )

    greet(twin)
    pl.when(chip != 7)(lambda: greet(above))
    pl.when(jnp.logical_or(chip == 0, chip >= 5))(lambda: greet(below))

    is_root = zero == ROOT

    @pl.when(is_root)
    def _():
        for other in range(16):
            if other != ROOT:
                greet(other)
        for far in (1, 2, 3):
            pl.semaphore_signal(
                barrier,
                inc=1,
                device_id={"cols": lax.rem(col + far, 4)},
                device_id_type=MESH,
            )

    for load in loads[3:]:
        load.start()

    def rows_of(origin, of, start=0, size=192):
        return pl.ds(pl.multiple_of(192 * (2 * origin + of) + start, 32), size)

    def slab(origin, of, start=0, size=384):
        return m_all.at[
            origin, pl.ds(pl.multiple_of(384 * of + start, 64), size)
        ]

    def piece(name, origin, way=0):
        if name == "k":
            return w_all.at[rows_of(origin, core), pl.ds(0, 256)]
        if name == "vq":
            return w_all.at[rows_of(origin, core), pl.ds(256, 1024)]
        if name == "w":
            return w_all.at[rows_of(origin, core)]
        if name == "m":
            return slab(origin, core)
        if name == "w half":
            return w_all.at[rows_of(origin, core, 96 * way, 96)]
        middle = MIDDLE_OF_4 if name == "m part of 4" else MIDDLE
        return slab(
            origin, core, middle * way, 384 - middle if way else middle
        )

    slots = {
        0: {"k": 0, "vq": 1, "m": 2},
        1: {"w": 3, "m": 4},
        2: {"w": 5, "m": 6},
        3: {"w half": 7, "m half": 8, "m part of 4": 8},
    }

    def arrived_from(way, step):
        return lax.rem(chip + (7 - step if way == 0 else step + 1), 8)

    def copy_of(name, way, step, origin, to):
        ref = piece(name, origin, way)
        return pltpu.make_async_remote_copy(
            src_ref=ref,
            dst_ref=ref,
            send_sem=send_sem.at[way, 1 if name[0] == "m" else 0],
            recv_sem=recv_sem.at[way, slots[step][name]],
            device_id={"zero": to},
            device_id_type=MESH,
        )

    def send(name, way, step):
        origin = chip if step == 0 else arrived_from(way, step - 1)
        copy_of(name, way, step, origin, above if way == 0 else below).start()

    def arrive(name, way, step):
        origin = arrived_from(way, step)
        copy_of(name, way, step, origin, twin).wait_recv()
        hand(name, origin, way)

    def hand(name, origin, way=0):
        ref = piece(name, origin, way)
        kind = 1 if name[0] == "m" else 0
        pltpu.make_async_remote_copy(
            src_ref=ref,
            dst_ref=ref,
            send_sem=hand_sem.at[kind],
            recv_sem=take_sem.at[kind],
            device_id={"zero": twin},
            device_id_type=MESH,
        ).start()

    def drain(sem, *refs):
        for ref in refs:
            pltpu.make_async_copy(ref, ref, sem).wait()

    own = rows_of(chip, core)
    for i in (0, 1, 2):
        loads[i].wait()
    w_all[own, 0:256] = merged(wk_v[...], lk_v[...], hk_v[...])
    pair = [
        pltpu.make_async_remote_copy(
            src_ref=src,
            dst_ref=dst,
            send_sem=pair_sent.at[i],
            recv_sem=pair_sem.at[i],
            device_id={"zero": twin},
            device_id_type=MESH,
        )
        for i, (src, dst) in enumerate(
            ((wm.at[:, other_half], wm_v.at[my_rows]), (hm, hm_v.at[core]))
        )
    ]
    pl.semaphore_wait(
        barrier,
        1
        + jnp.where(chip == 0, 0, 1)
        + jnp.where(chip >= 4, 1, 0)
        + jnp.where(is_root, 3, 1),
    )

    def ready(peer, i):
        pl.semaphore_signal(
            ready_sem.at[i], inc=1, device_id={"zero": peer}, device_id_type=MESH
        )

    pl.when(jnp.logical_and(chip >= 1, chip <= 4))(lambda: ready(below, 0))
    pl.when(chip == 7)(lambda: ready(above, 1))
    first = chip == 0
    early = jnp.logical_and(chip >= 1, chip <= 3)
    late = chip >= 4

    @pl.when(first)
    def _():
        pl.semaphore_wait(ready_sem.at[0], 1)
        send("k", 0, 0)

    @pl.when(jnp.logical_not(first))
    def _():
        send("k", 1, 0)

    pl.when(late)(lambda: send("k", 0, 0))
    for copy in pair:
        copy.start()
    loads[3].wait()
    loads[4].wait()
    n_all[col, zero] = jnp.zeros((1, 128), F32)
    n_all[col, zero, :, 0:48] = nt_v[...] + ns_v[...]
    row_copy = pltpu.make_async_remote_copy(
        src_ref=n_all.at[col, zero],
        dst_ref=n_all.at[col, zero],
        send_sem=norm_sent.at[0],
        recv_sem=norm_sem.at[0],
        device_id={"zero": ROOT},
        device_id_type=MESH,
    )
    for i in (5, 6, 7):
        loads[i].wait()
    w_all[own, 256:512] = merged(wv_v[...], lv_v[...], hv_v[...])
    for i in (8, 9, 10):
        loads[i].wait()
    w_all[own, 512:1280] = merged(wq_v[...], lq_v[...], hq_v[...])

    @pl.when(jnp.logical_not(first))
    def _():
        send("vq", 1, 0)

    @pl.when(early)
    def _():
        pl.semaphore_wait(ready_sem.at[0], 1)
        send("k", 0, 0)

    send("vq", 0, 0)

    @pl.when(first)
    def _():
        pl.semaphore_wait(ready_sem.at[1], 1)
        send("k", 1, 0)
        send("vq", 1, 0)

    @pl.when(jnp.logical_not(is_root))
    def _():
        row_copy.start()

    hand("w", chip)

    for i in (11, 12, 13):
        loads[i].wait()
    twin_rows = pl.ds(pl.multiple_of(192 * (1 - core), 64), 192)
    for i, dst in enumerate((wm_v.at[twin_rows], hm_v.at[1 - core])):
        pltpu.make_async_remote_copy(
            src_ref=dst,
            dst_ref=dst,
            send_sem=pair_sent.at[i],
            recv_sem=pair_sem.at[i],
            device_id={"zero": twin},
            device_id_type=MESH,
        ).wait_recv()
    row = lax.broadcasted_iota(jnp.int32, (192, 384), 0)
    lane = lax.broadcasted_iota(jnp.int32, (192, 384), 1)
    high = sum(
        jnp.dot(
            hm_v[c], (lane == row + 192 * c).astype(BF16), preferred_element_type=F32
        )
        for c in (0, 1)
    ).astype(BF16)
    for i in (0, 1, 2):
        lanes = slice(128 * i, 128 * i + 128)
        base = wm_v[:, lanes].astype(F32).T
        m_all[chip, pl.ds(pl.multiple_of(384 * core + 128 * i, 128), 128)] = merged(
            base, lm_v[:, lanes], high
        )
    send("m", 0, 0)
    send("m", 1, 0)
    hand("m", chip)
    for copy in pair:
        copy.wait_send()

    def meet_columns():
        drain(norm_sem.at[0], n_all.at[0, 0:15])
        for far in (1, 2, 3):
            pltpu.make_async_remote_copy(
                src_ref=n_all.at[col],
                dst_ref=n_all.at[col],
                send_sem=norm_sent.at[1],
                recv_sem=norm_sem.at[1],
                device_id={"cols": lax.rem(col + far, 4)},
                device_id_type=MESH,
            ).start()

    def assemble():
        drain(norm_sem.at[1], n_all.at[0:3])
        at = lax.broadcasted_iota(jnp.int32, (1, 128), 1)
        for g in range(8):
            e = [n_all[i % 4, 2 * g + i // 4] for i in range(8)]
            r = [pltpu.roll(e[i], (48 * i) % 128, 1) for i in range(8)]
            n_wide[3 * g : 3 * g + 1, :] = jnp.where(
                at < 48, r[0], jnp.where(at < 96, r[1], r[2])
            )
            n_wide[3 * g + 1 : 3 * g + 2, :] = jnp.where(
                at < 16,
                r[2],
                jnp.where(at < 64, r[3], jnp.where(at < 112, r[4], r[5])),
            )
            n_wide[3 * g + 2 : 3 * g + 3, :] = jnp.where(
                at < 32, r[5], jnp.where(at < 80, r[6], r[7])
            )
        n_out[...] = n_wide[...].astype(BF16)

    def norm_copy(to):
        return pltpu.make_async_remote_copy(
            src_ref=n_out,
            dst_ref=n_out,
            send_sem=norm_sent.at[2],
            recv_sem=norm_sem.at[2],
            device_id={"zero": to},
            device_id_type=MESH,
        )

    def spread():
        for to in (0, 2, 14, 4, 12, 6, 10, 8):
            norm_copy(to).start()

    ways = (0, 1)
    for way in ways:
        arrive("k", way, 0)
    pl.when(is_root)(meet_columns)
    for way in ways:
        arrive("vq", way, 0)
        send("w", way, 1)
    pl.when(is_root)(assemble)
    for way in ways:
        arrive("m", way, 0)
        send("m", way, 1)
    pl.when(is_root)(spread)
    for way in ways:
        arrive("w", way, 1)
        send("w", way, 2)
    for way in ways:
        arrive("m", way, 1)
        send("m", way, 2)
    for way in ways:
        arrive("w", way, 2)
        send("w half", way, 3)
    for way, odd_one in zip(ways, (7, 1)):
        arrive("m", way, 2)
        pl.when(chip != odd_one)(lambda: send("m half", way, 3))
        pl.when(chip == odd_one)(lambda: send("m part of 4", way, 3))
    for way in ways:
        arrive("w half", way, 3)

    @pl.when(is_root)
    def _():
        drain(norm_sent.at[1], n_all.at[0:3])
        drain(norm_sent.at[2], m_all.at[0, 0:64])

    @pl.when(jnp.logical_not(is_root))
    def _():
        row_copy.wait_send()
        norm_copy(twin).wait_recv()

    @pl.when(jnp.logical_and(core == 0, jnp.logical_not(first)))
    def _():
        norm_copy(twin).start()
        norm_copy(twin).wait_send()

    def finish(name):
        for way in ways:
            arrive(name, way, 3)

    pl.when(jnp.logical_not(first))(lambda: finish("m half"))
    pl.when(first)(lambda: finish("m part of 4"))
    for way, odd_one, rows in ((0, 7, 152), (1, 1, 184)):
        drain(send_sem.at[way, 0], w_all.at[0:672])
        pl.when(chip != odd_one)(
            lambda: drain(send_sem.at[way, 1], m_all.at[0:7, 0:192])
        )
        pl.when(chip == odd_one)(
            lambda: drain(send_sem.at[way, 1], m_all.at[:, 0:rows])
        )
    for sem in (hand_sem, take_sem):
        drain(sem.at[0], w_all.at[0:1536])
        drain(sem.at[1], m_all.at[:, 0:384])


def store_kernel(*refs):
    pl.run_scoped(
        functools.partial(store, *refs), sem=pltpu.SemaphoreType.DMA((5,))
    )


def store(w, m, n, q_out, k_out, v_out, m_out, n_out, sem):
    parts = [(m.at[i], m_out.at[:, pl.ds(384 * i, 384)], 1) for i in range(8)]
    for i in range(4):
        rows = pl.ds(768 * i, 768)
        parts += [
            (w.at[rows, pl.ds(512, 768)], q_out.at[rows], 0),
            (w.at[rows, pl.ds(0, 256)], k_out.at[rows], 2),
            (w.at[rows, pl.ds(256, 256)], v_out.at[rows], 3),
        ]
    parts += [(n, n_out, 4)]
    for src, dst, i in parts:
        pltpu.make_async_copy(src, dst, sem.at[i]).start()
    for i, dst in enumerate((q_out, m_out, k_out, v_out, n_out)):
        pltpu.make_async_copy(dst, dst, sem.at[i]).wait()


def on_device(wq, lq, hq, wk, lk, hk, wv, lv, hv, wm, lm, hm, nt, ns):
    anywhere = pl.BlockSpec(memory_space=pltpu.HBM)
    onchip = pl.BlockSpec(memory_space=pltpu.VMEM)
    held = pl.pallas_call(
        gather_kernel,
        out_shape=(
            pltpu.VMEM((3072, 1280), BF16),
            pltpu.VMEM((8, 768, 384), BF16),
            pltpu.VMEM((24, 128), BF16),
        ),
        in_specs=[anywhere] * 14,
        out_specs=(onchip,) * 3,
        scratch_shapes=[
            pltpu.VMEM((192, 768), BF16),
            pltpu.VMEM((32, 192), BF16),
            pltpu.VMEM((32, 768), BF16),
            pltpu.VMEM((192, 256), BF16),
            pltpu.VMEM((32, 192), BF16),
            pltpu.VMEM((32, 256), BF16),
            pltpu.VMEM((192, 256), BF16),
            pltpu.VMEM((32, 192), BF16),
            pltpu.VMEM((32, 256), BF16),
            pltpu.VMEM((384, 384), BF16),
            pltpu.VMEM((32, 384), BF16),
            pltpu.VMEM((2, 32, 192), BF16),
            pltpu.VMEM((1, 48), F32),
            pltpu.VMEM((1, 48), F32),
            pltpu.VMEM((4, 16, 1, 128), F32),
            pltpu.VMEM((24, 128), F32),
        ],
        compiler_params=pltpu.CompilerParams(
            collective_id=0, has_side_effects=True, vmem_limit_bytes=54400000
        ),
        name="merge_and_gather",
    )(
        wq, lq.T, hq, wk, lk.T, hk, wv, lv.T, hv, wm.T, lm.T, hm,
        nt.reshape(1, 48), ns.reshape(1, 48),
    )
    q, k, v, m, norm = pl.pallas_call(
        store_kernel,
        out_shape=(
            jax.ShapeDtypeStruct((3072, 768), BF16),
            jax.ShapeDtypeStruct((3072, 256), BF16),
            jax.ShapeDtypeStruct((3072, 256), BF16),
            jax.ShapeDtypeStruct((768, 3072), BF16),
            jax.ShapeDtypeStruct((24, 128), BF16),
        ),
        in_specs=[onchip] * 3,
        out_specs=(anywhere,) * 5,
        compiler_params=pltpu.CompilerParams(vmem_limit_bytes=24 * 2**20),
        name="store",
    )(*held)
    return q, k, v, m, norm.reshape(3072)


def solution(mesh):
    placed = (
        P(("job", "zero"), "cols"),
        P(("job", "zero"), None),
        P("job", "cols"),
        P(("job", "zero"), "cols"),
        P(("job", "zero"), None),
        P("job", "cols"),
        P(("job", "zero"), "cols"),
        P(("job", "zero"), None),
        P("job", "cols"),
        P(("job", "cols"), "zero"),
        P(("job", "cols"), None),
        P("job", "zero"),
        P(("job", "zero", "cols")),
        P(("job", "zero", "cols")),
    )
    return jax.shard_map(
        on_device,
        mesh=mesh,
        in_specs=placed,
        out_specs=(
            P("job", "cols"),
            P("job", "cols"),
            P("job", "cols"),
            P(("job", "cols"), None),
            P("job"),
        ),
        check_vma=False,
    )
```

```python
import functools

import jax
import jax.numpy as jnp
from jax import lax
from jax.experimental import pallas as pl
from jax.experimental.pallas import tpu as pltpu
from jax.sharding import PartitionSpec as P

mix_rate = 2.0
MESH = pl.DeviceIdType.MESH
BF16 = jnp.bfloat16
F32 = jnp.float32

ROOT = 1
SPLIT = {4: 80, 3: 320}
EVEN = 192
END = 64


def merged(base, low_turned, high):
    delta = lax.dot_general(
        low_turned, high, (((0,), (0,)), ((), ())), preferred_element_type=F32
    )
    return (base.astype(F32) + mix_rate * delta).astype(BF16)


def gather_kernel(*refs):
    pl.run_scoped(
        functools.partial(gather, *refs),
        load_sem=pltpu.SemaphoreType.DMA((14,)),
        pair_sent=pltpu.SemaphoreType.DMA((2,)),
        send_sem=pltpu.SemaphoreType.DMA((2, 2)),
        hand_sem=pltpu.SemaphoreType.DMA((2,)),
        norm_sent=pltpu.SemaphoreType.DMA((3,)),
        pair_sem=pltpu.SemaphoreType.DMA((2,)),
        recv_sem=pltpu.SemaphoreType.DMA((2, 10)),
        take_sem=pltpu.SemaphoreType.DMA((2,)),
        norm_sem=pltpu.SemaphoreType.DMA((3,)),
        ready_sem=pltpu.SemaphoreType.REGULAR((2,)),
    )


def gather(
    wq, lq, hq, wk, lk, hk, wv, lv, hv, wm, lm, hm, nt, ns,
    w_all, m_all, n_out,
    wq_v, lq_v, hq_v, wk_v, lk_v, hk_v, wv_v, lv_v, hv_v, wm_v, lm_v, hm_v, nt_v, ns_v,
    n_all, n_wide,
    load_sem, pair_sent, send_sem, hand_sem, norm_sent,
    pair_sem, recv_sem, take_sem, norm_sem, ready_sem,
):
    zero = lax.axis_index("zero")
    col = lax.axis_index("cols")
    core = lax.rem(zero, 2)
    chip = lax.div(zero, 2)
    above = lax.rem(zero + 2, 16)
    below = lax.rem(zero + 14, 16)
    twin = zero + 1 - 2 * core

    half = pl.ds(pl.multiple_of(384 * core, 128), 384)
    other_half = pl.ds(pl.multiple_of(384 * (1 - core), 128), 384)
    my_rows = pl.ds(pl.multiple_of(192 * core, 64), 192)
    loads = [
        pltpu.make_async_copy(src, dst, load_sem.at[i])
        for i, (src, dst) in enumerate(
            (
                (lk, lk_v),
                (hk, hk_v),
                (wk, wk_v),
                (nt, nt_v),
                (ns, ns_v),
                (lv, lv_v),
                (hv, hv_v),
                (wv, wv_v),
                (lq, lq_v),
                (hq, hq_v),
                (wq, wq_v),
                (hm, hm_v.at[core]),
                (wm.at[:, half], wm_v.at[my_rows]),
                (lm.at[:, half], lm_v),
            )
        )
    ]
    for load in loads[:3]:
        load.start()

    barrier = pltpu.get_barrier_semaphore()

    def greet(peer):
        pl.semaphore_signal(
            barrier, inc=1, device_id={"zero": peer}, device_id_type=MESH
        )

    greet(twin)
    pl.when(chip != 7)(lambda: greet(above))
    pl.when(jnp.logical_or(chip == 0, chip >= 5))(lambda: greet(below))

    is_root = zero == ROOT

    @pl.when(is_root)
    def _():
        for other in range(16):
            if other != ROOT:
                greet(other)
        for far in (1, 2, 3):
            pl.semaphore_signal(
                barrier,
                inc=1,
                device_id={"cols": lax.rem(col + far, 4)},
                device_id_type=MESH,
            )

    for load in loads[3:]:
        load.start()

    def rows_of(origin, of, start=0, size=192):
        return pl.ds(pl.multiple_of(192 * (2 * origin + of) + start, 32), size)

    def slab(origin, of, start=0, size=384):
        return m_all.at[
            origin, pl.ds(pl.multiple_of(384 * of + start, 16), size)
        ]

    def piece(name, origin, way=0):
        if name == "k":
            return w_all.at[rows_of(origin, core), pl.ds(0, 256)]
        if name == "vq":
            return w_all.at[rows_of(origin, core), pl.ds(256, 1024)]
        if name == "w":
            return w_all.at[rows_of(origin, core)]
        if name == "m":
            return slab(origin, core)
        if name == "w half":
            return w_all.at[rows_of(origin, core, 96 * way, 96)]
        start, size = last_rows(name, way)
        if name.endswith("end"):
            return slab(origin, core, start + size - END, END)
        return slab(origin, core, start, size - END)

    def last_rows(name, way):
        split = int(name.split()[1])
        return (split, 384 - split) if way else (0, split)

    def by_origin(origin, act):
        odd = origin < 0
        for o, split in SPLIT.items():
            pl.when(origin == o)(functools.partial(act, split))
            odd = jnp.logical_or(odd, origin == o)
        pl.when(jnp.logical_not(odd))(functools.partial(act, EVEN))

    slots = {
        0: {"k": 0, "vq": 1, "m": 2},
        1: {"w": 3, "m": 4},
        2: {"w": 5, "m": 6},
        3: {"w half": 7},
    }

    def arrived_from(way, step):
        return lax.rem(chip + (7 - step if way == 0 else step + 1), 8)

    def copy_of(name, way, step, origin, to):
        ref = piece(name, origin, way)
        return pltpu.make_async_remote_copy(
            src_ref=ref,
            dst_ref=ref,
            send_sem=send_sem.at[way, 1 if name[0] == "m" else 0],
            recv_sem=recv_sem.at[way, slots[step].get(name, 9 if "end" in name else 8)],
            device_id={"zero": to},
            device_id_type=MESH,
        )

    def send(name, way, step):
        origin = chip if step == 0 else arrived_from(way, step - 1)
        copy_of(name, way, step, origin, above if way == 0 else below).start()

    def arrive(name, way, step):
        origin = arrived_from(way, step)
        copy_of(name, way, step, origin, twin).wait_recv()
        hand(name, origin, way)

    def hand(name, origin, way=0):
        ref = piece(name, origin, way)
        kind = 1 if name[0] == "m" else 0
        pltpu.make_async_remote_copy(
            src_ref=ref,
            dst_ref=ref,
            send_sem=hand_sem.at[kind],
            recv_sem=take_sem.at[kind],
            device_id={"zero": twin},
            device_id_type=MESH,
        ).start()

    def drain(sem, *refs):
        for ref in refs:
            pltpu.make_async_copy(ref, ref, sem).wait()

    own = rows_of(chip, core)
    for i in (0, 1, 2):
        loads[i].wait()
    w_all[own, 0:256] = merged(wk_v[...], lk_v[...], hk_v[...])
    pair = [
        pltpu.make_async_remote_copy(
            src_ref=src,
            dst_ref=dst,
            send_sem=pair_sent.at[i],
            recv_sem=pair_sem.at[i],
            device_id={"zero": twin},
            device_id_type=MESH,
        )
        for i, (src, dst) in enumerate(
            ((wm.at[:, other_half], wm_v.at[my_rows]), (hm, hm_v.at[core]))
        )
    ]
    pl.semaphore_wait(
        barrier,
        1
        + jnp.where(chip == 0, 0, 1)
        + jnp.where(chip >= 4, 1, 0)
        + jnp.where(is_root, 3, 1),
    )

    def ready(peer, i):
        pl.semaphore_signal(
            ready_sem.at[i], inc=1, device_id={"zero": peer}, device_id_type=MESH
        )

    pl.when(jnp.logical_and(chip >= 1, chip <= 4))(lambda: ready(below, 0))
    pl.when(chip == 7)(lambda: ready(above, 1))
    first = chip == 0
    early = jnp.logical_and(chip >= 1, chip <= 3)
    late = chip >= 4

    @pl.when(first)
    def _():
        pl.semaphore_wait(ready_sem.at[0], 1)
        send("k", 0, 0)

    @pl.when(jnp.logical_not(first))
    def _():
        send("k", 1, 0)

    pl.when(late)(lambda: send("k", 0, 0))
    for copy in pair:
        copy.start()
    loads[3].wait()
    loads[4].wait()
    n_all[col, zero] = jnp.zeros((1, 128), F32)
    n_all[col, zero, :, 0:48] = nt_v[...] + ns_v[...]
    row_copy = pltpu.make_async_remote_copy(
        src_ref=n_all.at[col, zero],
        dst_ref=n_all.at[col, zero],
        send_sem=norm_sent.at[0],
        recv_sem=norm_sem.at[0],
        device_id={"zero": ROOT},
        device_id_type=MESH,
    )
    for i in (5, 6, 7):
        loads[i].wait()
    w_all[own, 256:512] = merged(wv_v[...], lv_v[...], hv_v[...])
    for i in (8, 9, 10):
        loads[i].wait()
    w_all[own, 512:1280] = merged(wq_v[...], lq_v[...], hq_v[...])

    @pl.when(jnp.logical_not(first))
    def _():
        send("vq", 1, 0)

    @pl.when(early)
    def _():
        pl.semaphore_wait(ready_sem.at[0], 1)
        send("k", 0, 0)

    send("vq", 0, 0)

    @pl.when(first)
    def _():
        pl.semaphore_wait(ready_sem.at[1], 1)
        send("k", 1, 0)
        send("vq", 1, 0)

    @pl.when(jnp.logical_not(is_root))
    def _():
        row_copy.start()

    hand("w", chip)

    for i in (11, 12, 13):
        loads[i].wait()
    twin_rows = pl.ds(pl.multiple_of(192 * (1 - core), 64), 192)
    for i, dst in enumerate((wm_v.at[twin_rows], hm_v.at[1 - core])):
        pltpu.make_async_remote_copy(
            src_ref=dst,
            dst_ref=dst,
            send_sem=pair_sent.at[i],
            recv_sem=pair_sem.at[i],
            device_id={"zero": twin},
            device_id_type=MESH,
        ).wait_recv()
    row = lax.broadcasted_iota(jnp.int32, (192, 384), 0)
    lane = lax.broadcasted_iota(jnp.int32, (192, 384), 1)
    high = sum(
        jnp.dot(
            hm_v[c], (lane == row + 192 * c).astype(BF16), preferred_element_type=F32
        )
        for c in (0, 1)
    ).astype(BF16)
    for i in (0, 1, 2):
        lanes = slice(128 * i, 128 * i + 128)
        base = wm_v[:, lanes].astype(F32).T
        m_all[chip, pl.ds(pl.multiple_of(384 * core + 128 * i, 128), 128)] = merged(
            base, lm_v[:, lanes], high
        )
    send("m", 0, 0)
    send("m", 1, 0)
    hand("m", chip)
    for copy in pair:
        copy.wait_send()

    def meet_columns():
        drain(norm_sem.at[0], n_all.at[0, 0:15])
        for far in (1, 2, 3):
            pltpu.make_async_remote_copy(
                src_ref=n_all.at[col],
                dst_ref=n_all.at[col],
                send_sem=norm_sent.at[1],
                recv_sem=norm_sem.at[1],
                device_id={"cols": lax.rem(col + far, 4)},
                device_id_type=MESH,
            ).start()

    def assemble():
        drain(norm_sem.at[1], n_all.at[0:3])
        at = lax.broadcasted_iota(jnp.int32, (1, 128), 1)
        for g in range(8):
            e = [n_all[i % 4, 2 * g + i // 4] for i in range(8)]
            r = [pltpu.roll(e[i], (48 * i) % 128, 1) for i in range(8)]
            n_wide[3 * g : 3 * g + 1, :] = jnp.where(
                at < 48, r[0], jnp.where(at < 96, r[1], r[2])
            )
            n_wide[3 * g + 1 : 3 * g + 2, :] = jnp.where(
                at < 16,
                r[2],
                jnp.where(at < 64, r[3], jnp.where(at < 112, r[4], r[5])),
            )
            n_wide[3 * g + 2 : 3 * g + 3, :] = jnp.where(
                at < 32, r[5], jnp.where(at < 80, r[6], r[7])
            )
        n_out[...] = n_wide[...].astype(BF16)

    def norm_copy(to):
        return pltpu.make_async_remote_copy(
            src_ref=n_out,
            dst_ref=n_out,
            send_sem=norm_sent.at[2],
            recv_sem=norm_sem.at[2],
            device_id={"zero": to},
            device_id_type=MESH,
        )

    def spread():
        for to in (0, 2, 14, 4, 12, 6, 10, 8):
            norm_copy(to).start()

    def send_last(way, split):
        for end in ("", " end"):
            if end or last_rows(f"m {split}", way)[1] > END:
                send(f"m {split}{end}", way, 3)

    def arrive_last(way, end, split):
        if end or last_rows(f"m {split}", way)[1] > END:
            arrive(f"m {split}{end}", way, 3)

    ways = (0, 1)
    for way in ways:
        arrive("k", way, 0)
    pl.when(is_root)(meet_columns)
    for way in ways:
        arrive("vq", way, 0)
        send("w", way, 1)
    pl.when(is_root)(assemble)
    for way in ways:
        arrive("m", way, 0)
        send("m", way, 1)
    pl.when(is_root)(spread)
    for way in ways:
        arrive("w", way, 1)
        send("w", way, 2)
    for way in ways:
        arrive("m", way, 1)
        send("m", way, 2)
    for way in ways:
        arrive("w", way, 2)
        send("w half", way, 3)
    for way in ways:
        arrive("m", way, 2)
        by_origin(arrived_from(way, 2), functools.partial(send_last, way))
    for way in ways:
        arrive("w half", way, 3)

    @pl.when(is_root)
    def _():
        drain(norm_sent.at[1], n_all.at[0:3])
        drain(norm_sent.at[2], m_all.at[0, 0:64])

    @pl.when(jnp.logical_not(is_root))
    def _():
        row_copy.wait_send()
        norm_copy(twin).wait_recv()

    @pl.when(jnp.logical_and(core == 0, jnp.logical_not(first)))
    def _():
        norm_copy(twin).start()
        norm_copy(twin).wait_send()

    for end in ("", " end"):
        for way in ways:
            by_origin(
                arrived_from(way, 3), functools.partial(arrive_last, way, end)
            )

    def drain_slabs(way, split):
        rows = 3 * 384 + last_rows(f"m {split}", way)[1]
        parts = next(p for p in (8, 6, 4, 2) if rows % (8 * p) == 0)
        drain(send_sem.at[way, 1], m_all.at[0:parts, 0 : rows // parts])

    for way in ways:
        drain(send_sem.at[way, 0], w_all.at[0:672])
        by_origin(arrived_from(way, 2), functools.partial(drain_slabs, way))
    for sem in (hand_sem, take_sem):
        drain(sem.at[0], w_all.at[0:1536])
        drain(sem.at[1], m_all.at[:, 0:384])


def store_kernel(w, m, n, q_out, k_out, v_out, m_out, n_out, sem):
    parts = [(m.at[i], m_out.at[:, pl.ds(384 * i, 384)], 1) for i in range(8)]
    for i in range(4):
        rows = pl.ds(768 * i, 768)
        parts += [
            (w.at[rows, pl.ds(512, 768)], q_out.at[rows], 0),
            (w.at[rows, pl.ds(0, 256)], k_out.at[rows], 2),
            (w.at[rows, pl.ds(256, 256)], v_out.at[rows], 3),
        ]
    parts += [(n, n_out, 4)]
    for src, dst, i in parts:
        pltpu.make_async_copy(src, dst, sem.at[i]).start()
    for i, dst in enumerate((q_out, m_out, k_out, v_out, n_out)):
        pltpu.make_async_copy(dst, dst, sem.at[i]).wait()


def on_device(wq, lq, hq, wk, lk, hk, wv, lv, hv, wm, lm, hm, nt, ns):
    anywhere = pl.BlockSpec(memory_space=pltpu.HBM)
    onchip = pl.BlockSpec(memory_space=pltpu.VMEM)
    held = pl.pallas_call(
        gather_kernel,
        out_shape=(
            pltpu.VMEM((3072, 1280), BF16),
            pltpu.VMEM((8, 768, 384), BF16),
            pltpu.VMEM((24, 128), BF16),
        ),
        in_specs=[anywhere] * 14,
        out_specs=(onchip,) * 3,
        scratch_shapes=[
            pltpu.VMEM((192, 768), BF16),
            pltpu.VMEM((32, 192), BF16),
            pltpu.VMEM((32, 768), BF16),
            pltpu.VMEM((192, 256), BF16),
            pltpu.VMEM((32, 192), BF16),
            pltpu.VMEM((32, 256), BF16),
            pltpu.VMEM((192, 256), BF16),
            pltpu.VMEM((32, 192), BF16),
            pltpu.VMEM((32, 256), BF16),
            pltpu.VMEM((384, 384), BF16),
            pltpu.VMEM((32, 384), BF16),
            pltpu.VMEM((2, 32, 192), BF16),
            pltpu.VMEM((1, 48), F32),
            pltpu.VMEM((1, 48), F32),
            pltpu.VMEM((4, 16, 1, 128), F32),
            pltpu.VMEM((24, 128), F32),
        ],
        compiler_params=pltpu.CompilerParams(
            collective_id=0, has_side_effects=True, vmem_limit_bytes=54400000
        ),
        name="merge_and_gather",
    )(
        wq, lq.T, hq, wk, lk.T, hk, wv, lv.T, hv, wm.T, lm.T, hm,
        nt.reshape(1, 48), ns.reshape(1, 48),
    )
    q, k, v, m, norm = pl.pallas_call(
        store_kernel,
        out_shape=(
            jax.ShapeDtypeStruct((3072, 768), BF16),
            jax.ShapeDtypeStruct((3072, 256), BF16),
            jax.ShapeDtypeStruct((3072, 256), BF16),
            jax.ShapeDtypeStruct((768, 3072), BF16),
            jax.ShapeDtypeStruct((24, 128), BF16),
        ),
        in_specs=[onchip] * 3,
        out_specs=(anywhere,) * 5,
        scratch_shapes=[pltpu.SemaphoreType.DMA((5,))],
        compiler_params=pltpu.CompilerParams(vmem_limit_bytes=24 * 2**20),
        name="store",
    )(*held)
    return q, k, v, m, norm.reshape(3072)


def solution(mesh):
    placed = (
        P(("job", "zero"), "cols"),
        P(("job", "zero"), None),
        P("job", "cols"),
        P(("job", "zero"), "cols"),
        P(("job", "zero"), None),
        P("job", "cols"),
        P(("job", "zero"), "cols"),
        P(("job", "zero"), None),
        P("job", "cols"),
        P(("job", "cols"), "zero"),
        P(("job", "cols"), None),
        P("job", "zero"),
        P(("job", "zero", "cols")),
        P(("job", "zero", "cols")),
    )
    return jax.shard_map(
        on_device,
        mesh=mesh,
        in_specs=placed,
        out_specs=(
            P("job", "cols"),
            P("job", "cols"),
            P("job", "cols"),
            P(("job", "cols"), None),
            P("job"),
        ),
        check_vma=False,
    )
```

```python
import functools

import jax
import jax.numpy as jnp
from jax import lax
from jax.experimental import pallas as pl
from jax.experimental.pallas import tpu as pltpu
from jax.sharding import PartitionSpec as P

mix_rate = 2.0
MESH = pl.DeviceIdType.MESH
BF16 = jnp.bfloat16
F32 = jnp.float32

ROOT = 1
MIDDLE, MIDDLE_OF_4 = 192, 64


def merged(base, low_turned, high):
    delta = lax.dot_general(
        low_turned, high, (((0,), (0,)), ((), ())), preferred_element_type=F32
    )
    return (base.astype(F32) + mix_rate * delta).astype(BF16)


def gather_kernel(*refs):
    pl.run_scoped(
        functools.partial(gather, *refs),
        load_sem=pltpu.SemaphoreType.DMA((14,)),
        pair_sent=pltpu.SemaphoreType.DMA((2,)),
        send_sem=pltpu.SemaphoreType.DMA((2, 2)),
        hand_sem=pltpu.SemaphoreType.DMA((2,)),
        norm_sent=pltpu.SemaphoreType.DMA((3,)),
        pair_sem=pltpu.SemaphoreType.DMA((2,)),
        recv_sem=pltpu.SemaphoreType.DMA((2, 9)),
        take_sem=pltpu.SemaphoreType.DMA((2,)),
        norm_sem=pltpu.SemaphoreType.DMA((3,)),
        ready_sem=pltpu.SemaphoreType.REGULAR((2,)),
    )


def gather(
    wq, lq, hq, wk, lk, hk, wv, lv, hv, wm, lm, hm, nt, ns,
    w_all, m_all, n_out,
    wq_v, lq_v, hq_v, wk_v, lk_v, hk_v, wv_v, lv_v, hv_v, wm_v, lm_v, hm_v, nt_v, ns_v,
    n_all, n_wide,
    load_sem, pair_sent, send_sem, hand_sem, norm_sent,
    pair_sem, recv_sem, take_sem, norm_sem, ready_sem,
):
    zero = lax.axis_index("zero")
    col = lax.axis_index("cols")
    core = lax.rem(zero, 2)
    chip = lax.div(zero, 2)
    above = lax.rem(zero + 2, 16)
    below = lax.rem(zero + 14, 16)
    twin = zero + 1 - 2 * core

    half = pl.ds(pl.multiple_of(384 * core, 128), 384)
    other_half = pl.ds(pl.multiple_of(384 * (1 - core), 128), 384)
    my_rows = pl.ds(pl.multiple_of(192 * core, 64), 192)
    loads = [
        pltpu.make_async_copy(src, dst, load_sem.at[i])
        for i, (src, dst) in enumerate(
            (
                (lk, lk_v),
                (hk, hk_v),
                (wk, wk_v),
                (nt, nt_v),
                (ns, ns_v),
                (lv, lv_v),
                (hv, hv_v),
                (wv, wv_v),
                (lq, lq_v),
                (hq, hq_v),
                (wq, wq_v),
                (hm, hm_v.at[core]),
                (wm.at[:, half], wm_v.at[my_rows]),
                (lm.at[:, half], lm_v),
            )
        )
    ]
    for load in loads[:3]:
        load.start()

    barrier = pltpu.get_barrier_semaphore()

    def greet(peer):
        pl.semaphore_signal(
            barrier, inc=1, device_id={"zero": peer}, device_id_type=MESH
        )

    greet(twin)
    pl.when(chip != 7)(lambda: greet(above))
    pl.when(jnp.logical_or(chip == 0, chip >= 5))(lambda: greet(below))

    is_root = zero == ROOT

    @pl.when(is_root)
    def _():
        for other in range(16):
            if other != ROOT:
                greet(other)
        for far in (1, 2, 3):
            pl.semaphore_signal(
                barrier,
                inc=1,
                device_id={"cols": lax.rem(col + far, 4)},
                device_id_type=MESH,
            )

    for load in loads[3:]:
        load.start()

    def rows_of(origin, of, start=0, size=192):
        return pl.ds(pl.multiple_of(192 * (2 * origin + of) + start, 32), size)

    def slab(origin, of, start=0, size=384):
        return m_all.at[
            origin, pl.ds(pl.multiple_of(384 * of + start, 64), size)
        ]

    def piece(name, origin, way=0):
        if name == "k":
            return w_all.at[rows_of(origin, core), pl.ds(0, 256)]
        if name == "vq":
            return w_all.at[rows_of(origin, core), pl.ds(256, 1024)]
        if name == "w":
            return w_all.at[rows_of(origin, core)]
        if name == "m":
            return slab(origin, core)
        if name == "w half":
            return w_all.at[rows_of(origin, core, 96 * way, 96)]
        middle = MIDDLE_OF_4 if name == "m part of 4" else MIDDLE
        return slab(
            origin, core, middle * way, 384 - middle if way else middle
        )

    slots = {
        0: {"k": 0, "vq": 1, "m": 2},
        1: {"w": 3, "m": 4},
        2: {"w": 5, "m": 6},
        3: {"w half": 7, "m half": 8, "m part of 4": 8},
    }

    def arrived_from(way, step):
        return lax.rem(chip + (7 - step if way == 0 else step + 1), 8)

    def copy_of(name, way, step, origin, to):
        ref = piece(name, origin, way)
        return pltpu.make_async_remote_copy(
            src_ref=ref,
            dst_ref=ref,
            send_sem=send_sem.at[way, 1 if name[0] == "m" else 0],
            recv_sem=recv_sem.at[way, slots[step][name]],
            device_id={"zero": to},
            device_id_type=MESH,
        )

    def send(name, way, step):
        origin = chip if step == 0 else arrived_from(way, step - 1)
        copy_of(name, way, step, origin, above if way == 0 else below).start()

    def arrive(name, way, step):
        origin = arrived_from(way, step)
        copy_of(name, way, step, origin, twin).wait_recv()
        hand(name, origin, way)

    def hand(name, origin, way=0):
        ref = piece(name, origin, way)
        kind = 1 if name[0] == "m" else 0
        pltpu.make_async_remote_copy(
            src_ref=ref,
            dst_ref=ref,
            send_sem=hand_sem.at[kind],
            recv_sem=take_sem.at[kind],
            device_id={"zero": twin},
            device_id_type=MESH,
        ).start()

    def drain(sem, *refs):
        for ref in refs:
            pltpu.make_async_copy(ref, ref, sem).wait()

    own = rows_of(chip, core)
    for i in (0, 1, 2):
        loads[i].wait()
    w_all[own, 0:256] = merged(wk_v[...], lk_v[...], hk_v[...])
    loads[3].wait()
    loads[4].wait()
    n_all[col, zero] = jnp.zeros((1, 128), F32)
    n_all[col, zero, :, 0:48] = nt_v[...] + ns_v[...]
    row_copy = pltpu.make_async_remote_copy(
        src_ref=n_all.at[col, zero],
        dst_ref=n_all.at[col, zero],
        send_sem=norm_sent.at[0],
        recv_sem=norm_sem.at[0],
        device_id={"zero": ROOT},
        device_id_type=MESH,
    )
    pair = [
        pltpu.make_async_remote_copy(
            src_ref=src,
            dst_ref=dst,
            send_sem=pair_sent.at[i],
            recv_sem=pair_sem.at[i],
            device_id={"zero": twin},
            device_id_type=MESH,
        )
        for i, (src, dst) in enumerate(
            ((wm.at[:, other_half], wm_v.at[my_rows]), (hm, hm_v.at[core]))
        )
    ]
    pl.semaphore_wait(
        barrier,
        1
        + jnp.where(chip == 0, 0, 1)
        + jnp.where(chip >= 4, 1, 0)
        + jnp.where(is_root, 3, 1),
    )

    def ready(peer, i):
        pl.semaphore_signal(
            ready_sem.at[i], inc=1, device_id={"zero": peer}, device_id_type=MESH
        )

    pl.when(jnp.logical_and(chip >= 1, chip <= 4))(lambda: ready(below, 0))
    pl.when(chip == 7)(lambda: ready(above, 1))
    first = chip == 0
    early = jnp.logical_and(chip >= 1, chip <= 3)
    late = chip >= 4

    @pl.when(first)
    def _():
        pl.semaphore_wait(ready_sem.at[0], 1)
        send("k", 0, 0)

    @pl.when(jnp.logical_not(first))
    def _():
        send("k", 1, 0)

    pl.when(late)(lambda: send("k", 0, 0))
    for copy in pair:
        copy.start()
    for i in (5, 6, 7):
        loads[i].wait()
    w_all[own, 256:512] = merged(wv_v[...], lv_v[...], hv_v[...])
    for i in (8, 9, 10):
        loads[i].wait()
    w_all[own, 512:1280] = merged(wq_v[...], lq_v[...], hq_v[...])

    @pl.when(jnp.logical_not(first))
    def _():
        send("vq", 1, 0)

    @pl.when(early)
    def _():
        pl.semaphore_wait(ready_sem.at[0], 1)
        send("k", 0, 0)

    send("vq", 0, 0)

    @pl.when(first)
    def _():
        pl.semaphore_wait(ready_sem.at[1], 1)
        send("k", 1, 0)
        send("vq", 1, 0)

    @pl.when(jnp.logical_not(is_root))
    def _():
        row_copy.start()

    hand("w", chip)

    for i in (11, 12, 13):
        loads[i].wait()
    twin_rows = pl.ds(pl.multiple_of(192 * (1 - core), 64), 192)
    for i, dst in enumerate((wm_v.at[twin_rows], hm_v.at[1 - core])):
        pltpu.make_async_remote_copy(
            src_ref=dst,
            dst_ref=dst,
            send_sem=pair_sent.at[i],
            recv_sem=pair_sem.at[i],
            device_id={"zero": twin},
            device_id_type=MESH,
        ).wait_recv()
    row = lax.broadcasted_iota(jnp.int32, (192, 384), 0)
    lane = lax.broadcasted_iota(jnp.int32, (192, 384), 1)
    high = sum(
        jnp.dot(
            hm_v[c], (lane == row + 192 * c).astype(BF16), preferred_element_type=F32
        )
        for c in (0, 1)
    ).astype(BF16)
    for i in (0, 1, 2):
        lanes = slice(128 * i, 128 * i + 128)
        base = wm_v[:, lanes].astype(F32).T
        m_all[chip, pl.ds(pl.multiple_of(384 * core + 128 * i, 128), 128)] = merged(
            base, lm_v[:, lanes], high
        )
    send("m", 0, 0)
    send("m", 1, 0)
    hand("m", chip)
    for copy in pair:
        copy.wait_send()

    def meet_columns():
        drain(norm_sem.at[0], n_all.at[0, 0:15])
        for far in (1, 2, 3):
            pltpu.make_async_remote_copy(
                src_ref=n_all.at[col],
                dst_ref=n_all.at[col],
                send_sem=norm_sent.at[1],
                recv_sem=norm_sem.at[1],
                device_id={"cols": lax.rem(col + far, 4)},
                device_id_type=MESH,
            ).start()

    def assemble():
        drain(norm_sem.at[1], n_all.at[0:3])
        at = lax.broadcasted_iota(jnp.int32, (1, 128), 1)
        for g in range(8):
            e = [n_all[i % 4, 2 * g + i // 4] for i in range(8)]
            r = [pltpu.roll(e[i], (48 * i) % 128, 1) for i in range(8)]
            n_wide[3 * g : 3 * g + 1, :] = jnp.where(
                at < 48, r[0], jnp.where(at < 96, r[1], r[2])
            )
            n_wide[3 * g + 1 : 3 * g + 2, :] = jnp.where(
                at < 16,
                r[2],
                jnp.where(at < 64, r[3], jnp.where(at < 112, r[4], r[5])),
            )
            n_wide[3 * g + 2 : 3 * g + 3, :] = jnp.where(
                at < 32, r[5], jnp.where(at < 80, r[6], r[7])
            )
        n_out[...] = n_wide[...].astype(BF16)

    def norm_copy(to):
        return pltpu.make_async_remote_copy(
            src_ref=n_out,
            dst_ref=n_out,
            send_sem=norm_sent.at[2],
            recv_sem=norm_sem.at[2],
            device_id={"zero": to},
            device_id_type=MESH,
        )

    def spread():
        for to in (0, 2, 14, 4, 12, 6, 10, 8):
            norm_copy(to).start()

    ways = (0, 1)
    for way in ways:
        arrive("k", way, 0)
    pl.when(is_root)(meet_columns)
    for way in ways:
        arrive("vq", way, 0)
        send("w", way, 1)
    pl.when(is_root)(assemble)
    for way in ways:
        arrive("m", way, 0)
        send("m", way, 1)
    pl.when(is_root)(spread)
    for way in ways:
        arrive("w", way, 1)
        send("w", way, 2)
    for way in ways:
        arrive("m", way, 1)
        send("m", way, 2)
    for way in ways:
        arrive("w", way, 2)
        send("w half", way, 3)
    for way, odd_one in zip(ways, (7, 1)):
        arrive("m", way, 2)
        pl.when(chip != odd_one)(lambda: send("m half", way, 3))
        pl.when(chip == odd_one)(lambda: send("m part of 4", way, 3))
    for way in ways:
        arrive("w half", way, 3)

    @pl.when(is_root)
    def _():
        drain(norm_sent.at[1], n_all.at[0:3])
        drain(norm_sent.at[2], m_all.at[0, 0:64])

    @pl.when(jnp.logical_not(is_root))
    def _():
        row_copy.wait_send()
        norm_copy(twin).wait_recv()

    @pl.when(jnp.logical_and(core == 0, jnp.logical_not(first)))
    def _():
        norm_copy(twin).start()
        norm_copy(twin).wait_send()

    def finish(name):
        for way in ways:
            arrive(name, way, 3)

    pl.when(jnp.logical_not(first))(lambda: finish("m half"))
    pl.when(first)(lambda: finish("m part of 4"))
    for way, odd_one, rows in ((0, 7, 152), (1, 1, 184)):
        drain(send_sem.at[way, 0], w_all.at[0:672])
        pl.when(chip != odd_one)(
            lambda: drain(send_sem.at[way, 1], m_all.at[0:7, 0:192])
        )
        pl.when(chip == odd_one)(
            lambda: drain(send_sem.at[way, 1], m_all.at[:, 0:rows])
        )
    for sem in (hand_sem, take_sem):
        drain(sem.at[0], w_all.at[0:1536])
        drain(sem.at[1], m_all.at[:, 0:384])


def store_kernel(w, m, n, q_out, k_out, v_out, m_out, n_out, sem):
    parts = [(n, n_out, 4)]
    for i in range(16):
        rows, slab_rows = pl.ds(192 * i, 192), pl.ds(384 * (i % 2), 384)
        parts += [
            (w.at[rows, pl.ds(512, 768)], q_out.at[rows], 0),
            (
                m.at[i // 2, slab_rows],
                m_out.at[slab_rows, pl.ds(384 * (i // 2), 384)],
                1,
            ),
            (w.at[rows, pl.ds(0, 256)], k_out.at[rows], 2),
            (w.at[rows, pl.ds(256, 256)], v_out.at[rows], 3),
        ]
    for src, dst, i in parts:
        pltpu.make_async_copy(src, dst, sem.at[i]).start()
    for i, dst in enumerate((q_out, m_out, k_out, v_out, n_out)):
        pltpu.make_async_copy(dst, dst, sem.at[i]).wait()


def on_device(wq, lq, hq, wk, lk, hk, wv, lv, hv, wm, lm, hm, nt, ns):
    anywhere = pl.BlockSpec(memory_space=pltpu.HBM)
    onchip = pl.BlockSpec(memory_space=pltpu.VMEM)
    held = pl.pallas_call(
        gather_kernel,
        out_shape=(
            pltpu.VMEM((3072, 1280), BF16),
            pltpu.VMEM((8, 768, 384), BF16),
            pltpu.VMEM((24, 128), BF16),
        ),
        in_specs=[anywhere] * 14,
        out_specs=(onchip,) * 3,
        scratch_shapes=[
            pltpu.VMEM((192, 768), BF16),
            pltpu.VMEM((32, 192), BF16),
            pltpu.VMEM((32, 768), BF16),
            pltpu.VMEM((192, 256), BF16),
            pltpu.VMEM((32, 192), BF16),
            pltpu.VMEM((32, 256), BF16),
            pltpu.VMEM((192, 256), BF16),
            pltpu.VMEM((32, 192), BF16),
            pltpu.VMEM((32, 256), BF16),
            pltpu.VMEM((384, 384), BF16),
            pltpu.VMEM((32, 384), BF16),
            pltpu.VMEM((2, 32, 192), BF16),
            pltpu.VMEM((1, 48), F32),
            pltpu.VMEM((1, 48), F32),
            pltpu.VMEM((4, 16, 1, 128), F32),
            pltpu.VMEM((24, 128), F32),
        ],
        compiler_params=pltpu.CompilerParams(
            collective_id=0, has_side_effects=True, vmem_limit_bytes=54400000
        ),
        name="merge_and_gather",
    )(
        wq, lq.T, hq, wk, lk.T, hk, wv, lv.T, hv, wm.T, lm.T, hm,
        nt.reshape(1, 48), ns.reshape(1, 48),
    )
    q, k, v, m, norm = pl.pallas_call(
        store_kernel,
        out_shape=(
            jax.ShapeDtypeStruct((3072, 768), BF16),
            jax.ShapeDtypeStruct((3072, 256), BF16),
            jax.ShapeDtypeStruct((3072, 256), BF16),
            jax.ShapeDtypeStruct((768, 3072), BF16),
            jax.ShapeDtypeStruct((24, 128), BF16),
        ),
        in_specs=[onchip] * 3,
        out_specs=(anywhere,) * 5,
        scratch_shapes=[pltpu.SemaphoreType.DMA((5,))],
        compiler_params=pltpu.CompilerParams(vmem_limit_bytes=24 * 2**20),
        name="store",
    )(*held)
    return q, k, v, m, norm.reshape(3072)


def solution(mesh):
    placed = (
        P(("job", "zero"), "cols"),
        P(("job", "zero"), None),
        P("job", "cols"),
        P(("job", "zero"), "cols"),
        P(("job", "zero"), None),
        P("job", "cols"),
        P(("job", "zero"), "cols"),
        P(("job", "zero"), None),
        P("job", "cols"),
        P(("job", "cols"), "zero"),
        P(("job", "cols"), None),
        P("job", "zero"),
        P(("job", "zero", "cols")),
        P(("job", "zero", "cols")),
    )
    return jax.shard_map(
        on_device,
        mesh=mesh,
        in_specs=placed,
        out_specs=(
            P("job", "cols"),
            P("job", "cols"),
            P("job", "cols"),
            P(("job", "cols"), None),
            P("job"),
        ),
        check_vma=False,
    )
```
